16 devices in a mesh: rep: 1, dp: 16 (over x, y, z, core).
Axes of the slice: x: 2, y: 2, z: 2, core: 2. Of those that a mesh axis runs over, the one named last changes fastest.
Arguments:
- x: bfloat16 [16, 2048, 1024], P(('rep', 'dp'))
- dy: bfloat16 [16, 2048, 1024], P(('rep', 'dp'))
- w_gate: bfloat16 [2, 1024, 3200], replicated
- w_up: bfloat16 [2, 1024, 3200], replicated
- w_down: bfloat16 [2, 3200, 1024], replicated
- m_w_gate: float32 [2, 1024, 3200], replicated
- m_w_up: float32 [2, 1024, 3200], replicated
- m_w_down: float32 [2, 3200, 1024], replicated
- v_w_gate: float32 [2, 1024, 3200], replicated
- v_w_up: float32 [2, 1024, 3200], replicated
- v_w_down: float32 [2, 3200, 1024], replicated
Outputs:
- output 1: bfloat16 [2, 1024, 3200], P('rep')
- output 2: bfloat16 [2, 1024, 3200], P('rep')
- output 3: bfloat16 [2, 3200, 1024], P('rep')
- output 4: float32 [2, 1024, 3200], P('rep')
- output 5: float32 [2, 1024, 3200], P('rep')
- output 6: float32 [2, 3200, 1024], P('rep')
- output 7: float32 [2, 1024, 3200], P('rep')
- output 8: float32 [2, 1024, 3200], P('rep')
- output 9: float32 [2, 3200, 1024], P('rep')
All inputs are finite; a program needn't handle non-finite values.
Results may differ from the reference program's by a relative error of at most 0.022.
Values are sent between devices in bfloat16 or wider.
A program may use at most 2.75 GiB of HBM per device.

```python
import jax
import jax.numpy as jnp
from jax import lax

SEQUENCES = 16
TOKENS = 2048
D = 1024
FF = 3200
LAYERS = 2
NAMES = ("w_gate", "w_up", "w_down")
SHAPES = {"w_gate": (LAYERS, D, FF), "w_up": (LAYERS, D, FF), "w_down": (LAYERS, FF, D)}


def bump(key, n, height):
    away = (jnp.arange(n, dtype=jnp.int32) - jax.random.randint(key, (), 0, n, jnp.int32)) % n
    return jnp.where(away < n // 8, height, 1.0)


def together(key, own, strength):
    shared = jax.random.normal(key, own.shape[1:], jnp.float32)
    return (own + strength * shared) * lax.rsqrt(1 + strength * strength)


def setup_inputs(seed: int = 0, part: int = 0) -> dict:
    kx, kdy, ka, kb, kz, kf, kh, kl, *keys = jax.random.split(jax.random.key(seed), 8 + 3 * len(NAMES))
    kx, kdy, ka, kb = (jax.random.fold_in(k, part) for k in (kx, kdy, ka, kb))
    kw, km, kv = (keys[i::3] for i in range(3))
    shape = (SEQUENCES, TOKENS, D)
    much_x, much_dy = jax.random.uniform(kz, (2,), jnp.float32, 0.0, 1.0)
    loud = 2.0 ** jax.random.uniform(jax.random.fold_in(kz, 1), (), jnp.float32, -1.0, 2.0)
    layers = 2.0 ** jax.random.uniform(kl, (LAYERS, 1, 1), jnp.float32, -1.0, 1.0)
    x = together(ka, jax.random.normal(kx, shape, jnp.float32), much_x) * bump(kf, D, 4.0)
    dy = together(kb, jax.random.normal(kdy, shape, jnp.float32), much_dy)
    drawn = {"x": x.astype(jnp.bfloat16), "dy": (loud * dy * (SEQUENCES * TOKENS) ** -0.5).astype(jnp.bfloat16)}
    for key, name in zip(kw, NAMES, strict=True):
        w = jax.random.normal(key, SHAPES[name], jnp.float32) * SHAPES[name][1] ** -0.5
        drawn[name] = (w * {"w_gate": 1.0, "w_up": bump(kh, FF, 4.0), "w_down": layers}[name]).astype(jnp.bfloat16)
    for key, name in zip(km, NAMES, strict=True):
        drawn[f"m_{name}"] = 0.1 * jax.random.normal(key, SHAPES[name], jnp.float32)
    for key, name in zip(kv, NAMES, strict=True):
        drawn[f"v_{name}"] = jax.random.uniform(key, SHAPES[name], jnp.float32, 0.005, 0.015)
    return drawn


def matmul(a, w):
    return jnp.dot(a, w, preferred_element_type=jnp.float32).astype(jnp.bfloat16)


def normed(h):
    wide = h.astype(jnp.float32)
    scale = lax.rsqrt(jnp.mean(wide**2, -1, keepdims=True) + 1e-6)
    return (wide * scale).astype(jnp.bfloat16)


def layer(h, w):
    a = normed(h)
    gate = jnp.dot(a, w["w_gate"], preferred_element_type=jnp.float32)
    up = jnp.dot(a, w["w_up"], preferred_element_type=jnp.float32)
    return h + matmul((jax.nn.silu(gate) * up).astype(jnp.bfloat16), w["w_down"])


def adamw(w, m, v, g):
    m = 0.9 * m + 0.1 * g
    v = 0.95 * v + 0.05 * g * g
    step = m * lax.rsqrt(v + 1e-8) + 0.1 * w
    return (w - 0.02 * step).astype(jnp.bfloat16), m, v


def stack(weights, h):
    return lax.scan(lambda h, w: (layer(h, w), None), h, weights)[0]


def reference(x, dy, w_gate, w_up, w_down, m_w_gate, m_w_up, m_w_down, v_w_gate, v_w_up, v_w_down):
    weights = dict(zip(NAMES, (w_gate, w_up, w_down), strict=True))

    def take(so_far, sequence):
        h, by_y = sequence
        _, back = jax.vjp(lambda w: stack(w, h), weights)
        return jax.tree.map(lambda total, term: total + term.astype(jnp.float32), so_far, back(by_y)[0]), None

    none_yet = {name: jnp.zeros(w.shape, jnp.float32) for name, w in weights.items()}
    by_weights, _ = lax.scan(take, none_yet, (x, dy))
    gradients = [by_weights[name].astype(jnp.bfloat16).astype(jnp.float32) for name in NAMES]
    new = [
        adamw(w.astype(jnp.float32), m, v, g)
        for w, m, v, g in zip((w_gate, w_up, w_down), (m_w_gate, m_w_up, m_w_down), (v_w_gate, v_w_up, v_w_down), gradients, strict=True)
    ]
    return tuple(one[which] for which in range(3) for one in new)
```

```python
import jax
import jax.numpy as jnp
from jax import lax
from jax.experimental import pallas as pl
from jax.experimental.pallas import tpu as pltpu
from jax.sharding import PartitionSpec as P

BF, F32 = jnp.bfloat16, jnp.float32
T, D, FF = 2048, 1024, 3200
FC = 640
NF = FF // FC
NC = 2 * NF
TB = 512
NT = T // TB
VMEM_LIMIT = 63 * 2**20

AXES = (1, 8, 4, 2)
ORDER = ((1, 8, 4, 2), (1, 4, 2, 8), (1, 2, 8, 4))


def dot(a, b, ca, cb):
    return lax.dot_general(a, b, (((ca,), (cb,)), ((), ())), preferred_element_type=F32)


def inverse_rms(wide):
    return lax.rsqrt(jnp.mean(wide * wide, -1, keepdims=True) + 1e-6)


def hidden_back(gate, up, by_hidden):
    s = 1.0 / (1.0 + jnp.exp(-gate))
    silu = gate * s
    hidden = (silu * up).astype(BF)
    by_gate = (by_hidden * up * (s + silu * (1.0 - s))).astype(BF)
    by_up = (by_hidden * silu).astype(BF)
    return hidden, by_gate, by_up


def any_spec(n):
    return [pl.BlockSpec(memory_space=pl.ANY)] * n


def forward_kernel(x_ref, wg, wu, wd, gu0, h1_ref, a1_ref, a1t_ref, a0t_ref, wgu, wdv, hid, gub, wsem, dsem, osem):
    i = pl.program_id(0)

    def weights(c):
        cols = pl.ds(pl.multiple_of(c * FC, 128), FC)
        return (
            pltpu.make_async_copy(wg.at[0, :, cols], wgu.at[c, :, pl.ds(0, FC)], wsem.at[c, 0]),
            pltpu.make_async_copy(wu.at[0, :, cols], wgu.at[c, :, pl.ds(FC, FC)], wsem.at[c, 1]),
        )

    down = pltpu.make_async_copy(wd.at[0], wdv, dsem)

    @pl.when(i == 0)
    def _():
        for c in range(NF):
            for copy in weights(c):
                copy.start()
        down.start()

    def out_copy(c, row_block):
        rows = pl.ds(pl.multiple_of(row_block * TB, TB), TB)
        return pltpu.make_async_copy(gub.at[lax.rem(c, 2)], gu0.at[c, rows, :], osem.at[lax.rem(c, 2)])

    wide = x_ref[...].astype(F32)
    a0 = (wide * inverse_rms(wide)).astype(BF)
    a0t_ref[...] = a0.T
    a1_ref[...] = a0

    def chunk(c, carry):
        @pl.when(i == 0)
        def _():
            for copy in weights(c):
                copy.wait()

        @pl.when(c >= 2)
        def _():
            out_copy(c, i).wait()

        gu = dot(a1_ref[...], wgu[c], 1, 0)
        gub[lax.rem(c, 2)] = gu
        gate = gu[:, :FC]
        hid[:, pl.ds(pl.multiple_of(c * FC, 128), FC)] = (gate * (1.0 / (1.0 + jnp.exp(-gate))) * gu[:, FC:]).astype(BF)
        out_copy(c, i).start()
        return carry

    lax.fori_loop(0, NF, chunk, 0)

    @pl.when(i == 0)
    def _():
        down.wait()

    h1 = (wide + dot(hid[...], wdv[...], 1, 0).astype(BF).astype(F32)).astype(BF)
    h1_ref[...] = h1
    wide1 = h1.astype(F32)
    a1 = (wide1 * inverse_rms(wide1)).astype(BF)
    a1_ref[...] = a1
    a1t_ref[...] = a1.T
    out_copy(NF - 2, i).wait()
    out_copy(NF - 1, i).wait()


def forward(x, wg, wu, wd):
    rows = pl.BlockSpec((TB, D), lambda i: (i, 0))
    columns = pl.BlockSpec((D, TB), lambda i: (0, i))
    return pl.pallas_call(
        forward_kernel,
        grid=(NT,),
        out_shape=[
            jax.ShapeDtypeStruct((NF, T, 2 * FC), F32),
            jax.ShapeDtypeStruct((T, D), BF),
            jax.ShapeDtypeStruct((T, D), BF),
            jax.ShapeDtypeStruct((D, T), BF),
            jax.ShapeDtypeStruct((D, T), BF),
        ],
        in_specs=[rows] + any_spec(3),
        out_specs=any_spec(1) + [rows, rows, columns, columns],
        scratch_shapes=[
            pltpu.VMEM((NF, D, 2 * FC), BF),
            pltpu.VMEM((FF, D), BF),
            pltpu.VMEM((TB, FF), BF),
            pltpu.VMEM((2, TB, 2 * FC), F32),
            pltpu.SemaphoreType.DMA((NF, 2)),
            pltpu.SemaphoreType.DMA,
            pltpu.SemaphoreType.DMA((2,)),
        ],
        compiler_params=pltpu.CompilerParams(dimension_semantics=("arbitrary",), vmem_limit_bytes=VMEM_LIMIT),
        cost_estimate=pl.CostEstimate(flops=6 * T * D * FF, bytes_accessed=100 * 2**20, transcendentals=T * FF),
        name="forward",
    )(x, wg, wu, wd)


def at(x, m):
    return x if isinstance(x, int) else pl.multiple_of(x, m)


class Sum:
    def __init__(self, g, out, recv_gate_up, recv_down, recv_down_ici, send, recv, local, free):
        self.g, self.out = g, out
        self.recv_gate_up, self.recv_down, self.recv_down_ici = recv_gate_up, recv_down, recv_down_ici
        self.send, self.recv, self.local, self.free = send, recv, local, free
        self.me = lax.axis_index("dp")

    def bit(self, b):
        return lax.rem(self.me // b, 2)

    def peer(self, b):
        return self.me + b * (1 - 2 * self.bit(b))

    def barrier(self):
        barrier = pltpu.get_barrier_semaphore()
        for b in AXES:
            pl.semaphore_signal(barrier, inc=1, device_id={"dp": self.peer(b)})
        pl.semaphore_wait(barrier, len(AXES))

    def origin(self, p, level, other=False):
        row, column = 0, 0
        for k in range(level):
            h = self.bit(ORDER[p][k])
            if other and k == level - 1:
                h = 1 - h
            if p < 2:
                row = row + h * (D // 2 >> k)
            elif k == 0:
                row = row + h * (FC // 2)
            else:
                column = column + h * (D >> k)
        return row, column

    def shape(self, p, level):
        return (D >> level, FC) if p < 2 else (FC // 2, D >> (level - 1))

    def window(self, ref, origin, shape):
        return ref.at[pl.ds(at(origin[0], 64), shape[0]), pl.ds(at(origin[1], 128), shape[1])]

    def landing(self, p, k, slot):
        if p < 2:
            return self.recv_gate_up[p].at[slot, pl.ds(D - (D >> k), D // 2 >> k), :]
        if k == 0:
            return self.recv_down.at[slot]
        return self.recv_down_ici.at[slot, :, pl.ds(D - (D >> (k - 1)), D >> k)]

    def halve(self, p, c, k):
        slot = lax.rem(c, 2)
        return pltpu.make_async_remote_copy(
            src_ref=self.window(self.g[p].at[slot], self.origin(p, k + 1, other=True), self.shape(p, k + 1)),
            dst_ref=self.landing(p, k, slot),
            send_sem=self.send.at[slot, p, k],
            recv_sem=self.recv.at[slot, p, k],
            device_id={"dp": self.peer(ORDER[p][k])},
        )

    def place(self, p, c, origin, shape):
        layer, start = 1 - c // NF, lax.rem(c, NF) * FC
        if p < 2:
            return self.out[p].at[layer, pl.ds(at(origin[0], 64), shape[0]), pl.ds(pl.multiple_of(start, 128), FC)]
        return self.out[p].at[layer, pl.ds(pl.multiple_of(start + origin[0], 64), shape[0]), pl.ds(at(origin[1], 128), shape[1])]

    def gather(self, p, c, j):
        slot, level = lax.rem(c, 2), 4 - j
        origin, shape = self.origin(p, level), self.shape(p, level)
        there = self.place(p, c, origin, shape)
        return pltpu.make_async_remote_copy(
            src_ref=self.window(self.g[p].at[slot], origin, shape) if j == 0 else there,
            dst_ref=there,
            send_sem=self.send.at[slot, p, 4 + j],
            recv_sem=self.recv.at[slot, p, 4 + j],
            device_id={"dp": self.peer(ORDER[p][3 - j])},
        )

    def keep(self, p, c):
        slot = lax.rem(c, 2)
        origin, shape = self.origin(p, 4), self.shape(p, 4)
        return pltpu.make_async_copy(self.window(self.g[p].at[slot], origin, shape), self.place(p, c, origin, shape), self.local.at[slot, p])

    def add(self, p, c, k):
        slot = lax.rem(c, 2)
        level = min(k + 1, 4)
        (row, column), shape = self.origin(p, level, other=k < 4), self.shape(p, level)
        ref = self.g[p]
        if p < 2:

            def block(i, carry):
                here = (slot, pl.ds(pl.multiple_of(row + i * 64, 64), 64), slice(None))
                total = ref[here].astype(F32)
                for j in range(k):
                    there = D - (D >> j) + row - self.origin(p, j + 1)[0] + i * 64
                    total = total + self.recv_gate_up[p][slot, pl.ds(pl.multiple_of(there, 64), 64), :].astype(F32)
                ref[here] = total.astype(BF)
                return carry

            lax.fori_loop(0, shape[0] // 64, block, 0)
        else:

            def block(i, carry):
                here = (slot, pl.ds(pl.multiple_of(row, 64), shape[0]), pl.ds(pl.multiple_of(column + i * 128, 128), 128))
                total = ref[here].astype(F32)
                for j in range(k):
                    there = column - self.origin(p, j + 1)[1] + i * 128
                    if j == 0:
                        total = total + self.recv_down[slot, :, pl.ds(pl.multiple_of(there, 128), 128)].astype(F32)
                    else:
                        there = there + D - (D >> (j - 1))
                        total = total + self.recv_down_ici[slot, :, pl.ds(pl.multiple_of(there, 128), 128)].astype(F32)
                ref[here] = total.astype(BF)
                return carry

            lax.fori_loop(0, shape[1] // 128, block, 0)

    def step(self, k, parts, c):
        if k == 0:

            @pl.when(jnp.logical_and(c >= 2, min(parts) == 0))
            def _():
                pl.semaphore_wait(self.free.at[0], 1)

        if k == 1:

            @pl.when(c >= 2)
            def _():
                for q in range(1, 4):
                    pl.semaphore_wait(self.free.at[q], 1)

        for p in parts:
            if 1 <= k <= 4:
                self.halve(p, c, k - 1).wait()
                self.add(p, c, k)
            if k < 4:
                self.halve(p, c, k).start()
            if k == 4:
                self.keep(p, c).start()
            if k == 5:
                self.keep(p, c).wait()
            if k >= 5:
                self.gather(p, c, k - 5).wait()
            if 4 <= k < 8:
                self.gather(p, c, k - 4).start()
        if k == 4:

            @pl.when(c < NC - 2)
            def _():
                for q, b in enumerate(AXES):
                    pl.semaphore_signal(self.free.at[q], inc=1, device_id={"dp": self.peer(b)})


AFTER = {
    2: ((2, 1), (7, 2)),
    4: ((3, 1),),
    5: ((4, 1), (8, 2)),
    6: ((5, 1), (0, 0)),
    7: ((6, 1), (1, 0)),
}


def backward_kernel(
    a1, a1t, a0t, dy, h1, gu0, wg, wu, wd,
    out_gate, out_up, out_down,
    a, at_, by_h, by_a, wgu, wdv, hid, dgu, g_gate, g_up, g_down, recv_gate, recv_up, recv_down, recv_down_ici,
    load_sem, w_sem, gu_sem, send, recv, local, free,
):
    total = Sum((g_gate, g_up, g_down), (out_gate, out_up, out_down), (recv_gate, recv_up), recv_down, recv_down_ici, send, recv, local, free)

    def weights(c, both):
        layer, start, slot = 1 - c // NF, lax.rem(c, NF) * FC, lax.rem(c, 2)
        columns = pl.ds(pl.multiple_of(start, 128), FC)
        copies = [pltpu.make_async_copy(wd.at[layer, pl.ds(pl.multiple_of(start, 64), FC), :], wdv.at[slot], w_sem.at[slot, 0])]
        if both:
            copies.append(pltpu.make_async_copy(wg.at[layer, :, columns], wgu.at[slot, :, pl.ds(0, FC)], w_sem.at[slot, 1]))
            copies.append(pltpu.make_async_copy(wu.at[layer, :, columns], wgu.at[slot, :, pl.ds(FC, FC)], w_sem.at[slot, 2]))
        return copies

    def kept(n):
        slot, c, t = lax.rem(n, 2), n // NT, lax.rem(n, NT)
        rows = pl.ds(pl.multiple_of(t * TB, TB), TB)
        return [
            pltpu.make_async_copy(
                gu0.at[c, rows, pl.ds(half * FC, FC)],
                by_a.at[pl.ds(pl.multiple_of((2 * slot + half) * TB, TB), TB), pl.ds(0, FC)],
                gu_sem.at[slot, half],
            )
            for half in range(2)
        ]

    load_dy = pltpu.make_async_copy(dy, by_h, load_sem.at[0])
    load_a = pltpu.make_async_copy(a1, a, load_sem.at[1])
    load_at = pltpu.make_async_copy(a1t, at_, load_sem.at[2])
    load_h1 = pltpu.make_async_copy(h1, a, load_sem.at[1])
    load_a0t = pltpu.make_async_copy(a0t, at_, load_sem.at[2])

    load_dy.start()
    load_a.start()
    for copy in weights(0, True):
        copy.start()
    load_at.start()
    by_a[...] = jnp.zeros_like(by_a)
    total.barrier()

    def sends(step, c):
        for k, back in AFTER.get(step, ()):
            if back == 0:
                total.step(k, (0, 1, 2), c)
            else:

                @pl.when(c >= back)
                def _(k=k, back=back):
                    total.step(k, (0, 1, 2), c - back)

    def rows_of(t):
        return pl.ds(pl.multiple_of(t * TB, TB), TB)

    def weight_gradients(c):
        slot = lax.rem(c, 2)
        g_down[slot] = dot(hid[...], by_h[...], 0, 0).astype(BF)
        sends(4, c)

        def block(m, carry):
            rows = pl.ds(pl.multiple_of(m * 512, 512), 512)
            both = dot(at_[rows, :], dgu[...], 1, 0).astype(BF)
            g_gate[slot, rows, :] = both[:, :FC]
            g_up[slot, rows, :] = both[:, FC:]

            @pl.when(m == 0)
            def _():
                sends(5, c)

            @pl.when(m == 1)
            def _():
                sends(6, c)

            return carry

        lax.fori_loop(0, 2, block, 0)

    def last_layer(c, carry):
        slot = lax.rem(c, 2)
        for copy in weights(c, True):
            copy.wait()

        @pl.when(c < NF - 1)
        def _():
            for copy in weights(c + 1, True):
                copy.start()

        @pl.when(c == NF - 1)
        def _():
            for copy in weights(c + 1, False):
                copy.start()

        @pl.when(c == 0)
        def _():
            load_dy.wait()
            load_a.wait()

        def block(t, carry):
            rows = rows_of(t)
            gu = dot(a[rows, :], wgu[slot], 1, 0)
            by_hidden = dot(by_h[rows, :], wdv[slot], 1, 1).astype(BF).astype(F32)
            hid[rows, :], dgu[rows, :FC], dgu[rows, FC:] = hidden_back(gu[:, :FC], gu[:, FC:], by_hidden)
            for n in range(NT):
                if n in AFTER:

                    @pl.when(t == n)
                    def _(n=n):
                        sends(n, c)

            return carry

        lax.fori_loop(0, NT, block, 0)

        @pl.when(c == 0)
        def _():
            load_at.wait()

        @pl.when(c == NF - 1)
        def _():
            load_h1.start()

        weight_gradients(c)

        @pl.when(c == NF - 1)
        def _():
            load_a0t.start()

        def input_block(t, carry):
            rows = rows_of(t)
            by_a[rows, :] += dot(dgu[rows, :], wgu[slot], 1, 1)

            @pl.when(t == 1)
            def _():
                sends(7, c)

            @pl.when(t == 3)
            def _():
                sends(8, c)

            return carry

        lax.fori_loop(0, NT, input_block, 0)
        return carry

    lax.fori_loop(0, NF, last_layer, 0)

    load_h1.wait()

    def norm_block(t, carry):
        rows = pl.ds(pl.multiple_of(t * 128, 128), 128)
        wide = a[rows, :].astype(F32)
        scale = inverse_rms(wide)
        by_normed = by_a[rows, :].astype(BF).astype(F32)
        through = by_normed * scale - wide * (scale * scale * scale * jnp.mean(by_normed * wide, -1, keepdims=True))
        by_h[rows, :] = (by_h[rows, :].astype(F32) + through.astype(BF).astype(F32)).astype(BF)
        return carry

    lax.fori_loop(0, T // 128, norm_block, 0)
    for copy in kept(0):
        copy.start()
    load_a0t.wait()

    def first_layer(c, carry):
        slot = lax.rem(c, 2)
        for copy in weights(c, False):
            copy.wait()

        @pl.when(c < NC - 1)
        def _():
            for copy in weights(c + 1, False):
                copy.start()

        def block(t, carry):
            rows = rows_of(t)
            n = (c - NF) * NT + t
            for copy in kept(n):
                copy.wait()

            @pl.when(n + 1 < NF * NT)
            def _():
                for copy in kept(n + 1):
                    copy.start()

            here = lax.rem(n, 2) * 2 * TB
            gate = by_a[pl.ds(pl.multiple_of(here, TB), TB), :FC]
            up = by_a[pl.ds(pl.multiple_of(here + TB, TB), TB), :FC]
            by_hidden = dot(by_h[rows, :], wdv[slot], 1, 1).astype(BF).astype(F32)
            hid[rows, :], dgu[rows, :FC], dgu[rows, FC:] = hidden_back(gate, up, by_hidden)
            for n in range(NT):
                if n in AFTER:

                    @pl.when(t == n)
                    def _(n=n):
                        sends(n, c)

            return carry

        lax.fori_loop(0, NT, block, 0)
        weight_gradients(c)
        sends(7, c)
        sends(8, c)
        return carry

    lax.fori_loop(NF, NC, first_layer, 0)
    for i in (NC, NC + 1):
        for step in range(9):
            for k, back in AFTER.get(step, ()):
                if i - back < NC:
                    total.step(k, (0, 1, 2), i - back)


def backward(a1, a1t, a0t, dy, h1, gu0, wg, wu, wd):
    dma = pltpu.SemaphoreType.DMA
    return pl.pallas_call(
        backward_kernel,
        out_shape=[jax.ShapeDtypeStruct((2, D, FF), BF), jax.ShapeDtypeStruct((2, D, FF), BF), jax.ShapeDtypeStruct((2, FF, D), BF)],
        in_specs=any_spec(9),
        out_specs=any_spec(3),
        scratch_shapes=[
            pltpu.VMEM((T, D), BF),
            pltpu.VMEM((D, T), BF),
            pltpu.VMEM((T, D), BF),
            pltpu.VMEM((T, D), F32),
            pltpu.VMEM((2, D, 2 * FC), BF),
            pltpu.VMEM((2, FC, D), BF),
            pltpu.VMEM((T, FC), BF),
            pltpu.VMEM((T, 2 * FC), BF),
            pltpu.VMEM((2, D, FC), BF),
            pltpu.VMEM((2, D, FC), BF),
            pltpu.VMEM((2, FC, D), BF),
            pltpu.VMEM((2, D - D // 16, FC), BF),
            pltpu.VMEM((2, D - D // 16, FC), BF),
            pltpu.VMEM((2, FC // 2, D), BF),
            pltpu.VMEM((2, FC // 2, D - D // 8), BF),
            dma((3,)),
            dma((2, 3)),
            dma((2, 2)),
            dma((2, 3, 8)),
            dma((2, 3, 8)),
            dma((2, 3)),
            pltpu.SemaphoreType.REGULAR((4,)),
        ],
        compiler_params=pltpu.CompilerParams(collective_id=0, has_side_effects=True, vmem_limit_bytes=VMEM_LIMIT),
        cost_estimate=pl.CostEstimate(flops=24 * T * D * FF, bytes_accessed=200 * 2**20, transcendentals=2 * T * FF),
        name="backward",
    )(a1, a1t, a0t, dy, h1, gu0, wg, wu, wd)


def adamw(w, m, v, g):
    m = 0.9 * m + 0.1 * g
    v = 0.95 * v + 0.05 * g * g
    step = m * lax.rsqrt(v + 1e-8) + 0.1 * w
    return (w - 0.02 * step).astype(BF), m, v


def solution(mesh):
    def step(x, dy, *arrays):
        weights, m, v = (arrays[i : i + 3] for i in (0, 3, 6))
        gu0, h1, a1, a1t, a0t = forward(x[0], *weights)
        gradients = backward(a1, a1t, a0t, dy[0], h1, gu0, *weights)
        new = [adamw(w.astype(F32), m, v, g.astype(F32)) for w, m, v, g in zip(weights, m, v, gradients, strict=True)]
        return tuple(one[which] for which in range(3) for one in new)

    return jax.shard_map(
        step,
        mesh=mesh,
        in_specs=(P(("rep", "dp"), None, None),) * 2 + (P(None, None, None),) * 9,
        out_specs=(P("rep", None, None),) * 9,
        check_vma=False,
    )
```

```python
import jax
import jax.numpy as jnp
from jax import lax
from jax.experimental import pallas as pl
from jax.experimental.pallas import tpu as pltpu
from jax.sharding import PartitionSpec as P

BF, F32 = jnp.bfloat16, jnp.float32
T, D, FF = 2048, 1024, 3200
FC = 640
NF = FF // FC
NC = 2 * NF
TB = 512
NT = T // TB
NG = NF + 1
NK = NC - NG
RS = 2
VMEM_LIMIT = 63 * 2**20

AXES = (1, 8, 4, 2)
ORDER = (AXES, (1, 4, 2, 8), (1, 2, 8, 4))


def dot(a, b, ca, cb):
    return lax.dot_general(a, b, (((ca,), (cb,)), ((), ())), preferred_element_type=F32)


def inverse_rms(wide):
    return lax.rsqrt(jnp.mean(wide * wide, -1, keepdims=True) + 1e-6)


def gated(gate, up):
    s = 1.0 / (1.0 + jnp.exp(-gate))
    silu = gate * s
    return (silu * up).astype(BF), up * (s + silu * (1.0 - s)), silu


def split(a, b):
    return (a // b, a % b) if isinstance(a, int) else (lax.div(a, jnp.int32(b)), lax.rem(a, jnp.int32(b)))


def layer_and_start(c):
    before, chunk = split(c, NF)
    return 1 - before, chunk * FC


def any_spec(n):
    return [pl.BlockSpec(memory_space=pl.ANY)] * n


def forward_kernel(x_ref, wg, wu, wd, by0, hid0, h1_ref, a1_ref, a0_ref, wgu, wdv, hid, byb, wsem, dsem, osem, hsem):
    i = pl.program_id(0)
    rows = pl.ds(pl.multiple_of(i * TB, TB), TB)

    def columns(c):
        return pl.ds(pl.multiple_of(c * FC, 128), FC)

    def weights(c):
        return (
            pltpu.make_async_copy(wg.at[0, :, columns(c)], wgu.at[c, :, pl.ds(0, FC)], wsem.at[c, 0]),
            pltpu.make_async_copy(wu.at[0, :, columns(c)], wgu.at[c, :, pl.ds(FC, FC)], wsem.at[c, 1]),
        )

    down = pltpu.make_async_copy(wd.at[0], wdv, dsem)

    @pl.when(i == 0)
    def _():
        for c in range(NF):
            for copy in weights(c):
                copy.start()
        down.start()

    def out_by(c):
        return pltpu.make_async_copy(byb.at[lax.rem(c, 2)], by0.at[c, rows, :], osem.at[lax.rem(c, 2)])

    def out_hid(c):
        return pltpu.make_async_copy(hid.at[:, columns(c)], hid0.at[c, rows, :], hsem.at[c])

    wide = x_ref[...].astype(F32)
    a0_ref[...] = (wide * inverse_rms(wide)).astype(BF)

    def chunk(c, carry):
        @pl.when(i == 0)
        def _():
            for copy in weights(c):
                copy.wait()

        @pl.when(c >= 2)
        def _():
            out_by(c).wait()

        gu = dot(a0_ref[...], wgu[c], 1, 0)
        hid[:, columns(c)], byb[lax.rem(c, 2), :, :FC], byb[lax.rem(c, 2), :, FC:] = gated(gu[:, :FC], gu[:, FC:])
        out_by(c).start()
        out_hid(c).start()
        return carry

    lax.fori_loop(0, NF, chunk, 0)

    @pl.when(i == 0)
    def _():
        down.wait()

    h1_ref[...] = (x_ref[...].astype(F32) + dot(hid[...], wdv[...], 1, 0).astype(BF).astype(F32)).astype(BF)
    wide1 = h1_ref[...].astype(F32)
    a1_ref[...] = (wide1 * inverse_rms(wide1)).astype(BF)
    for c in range(NF):
        out_hid(c).wait()
    out_by(NF - 2).wait()
    out_by(NF - 1).wait()


def forward(x, wg, wu, wd):
    rows = pl.BlockSpec((TB, D), lambda i: (i, 0))
    dma = pltpu.SemaphoreType.DMA
    return pl.pallas_call(
        forward_kernel,
        grid=(NT,),
        out_shape=[
            jax.ShapeDtypeStruct((NF, T, 2 * FC), F32),
            jax.ShapeDtypeStruct((NF, T, FC), BF),
            jax.ShapeDtypeStruct((T, D), BF),
            jax.ShapeDtypeStruct((T, D), BF),
            jax.ShapeDtypeStruct((T, D), BF),
        ],
        in_specs=[rows] + any_spec(3),
        out_specs=any_spec(2) + [rows] * 3,
        scratch_shapes=[
            pltpu.VMEM((NF, D, 2 * FC), BF),
            pltpu.VMEM((FF, D), BF),
            pltpu.VMEM((TB, FF), BF),
            pltpu.VMEM((2, TB, 2 * FC), F32),
            dma((NF, 2)),
            dma,
            dma((2,)),
            dma((NF,)),
        ],
        compiler_params=pltpu.CompilerParams(dimension_semantics=("arbitrary",), vmem_limit_bytes=VMEM_LIMIT),
        cost_estimate=pl.CostEstimate(flops=6 * T * D * FF, bytes_accessed=110 * 2**20, transcendentals=T * FF),
        name="forward",
    )(x, wg, wu, wd)


def at(x, m):
    return x if isinstance(x, int) else pl.multiple_of(x, m)


class Sum:
    def __init__(self, g, out, pieces, recv_gate_up, recv_down, recv_down_ici, send, recv, gather_send, gather_recv, local, free):
        self.g, self.out, self.pieces = g, out, pieces
        self.recv_gate_up, self.recv_down, self.recv_down_ici = recv_gate_up, recv_down, recv_down_ici
        self.send, self.recv, self.local, self.free = send, recv, local, free
        self.gather_send, self.gather_recv = gather_send, gather_recv
        me = lax.axis_index("dp")
        bits = {b: split(split(me, b)[0], 2)[1] for b in AXES}
        self.core = bits[1]
        self.peers = {b: me + b * (1 - 2 * bits[b]) for b in AXES}
        self.origins = {}
        for p in range(3):
            row = column = 0
            self.origins[p, 0, False] = row, column
            for k, b in enumerate(ORDER[p]):
                for other in (True, False):
                    h = 1 - bits[b] if other else bits[b]
                    if p < 2:
                        here = row + h * (D // 2 >> k), column
                    elif k == 0:
                        here = row + h * (FC // 2), column
                    else:
                        here = row, column + h * (D >> k)
                    self.origins[p, k + 1, other] = here
                row, column = here

    def peer(self, b):
        return self.peers[b]

    def arrive(self):
        for b in AXES:
            pl.semaphore_signal(pltpu.get_barrier_semaphore(), inc=1, device_id={"dp": self.peer(b)})

    def meet(self):
        pl.semaphore_wait(pltpu.get_barrier_semaphore(), len(AXES))

    def origin(self, p, level, other=False):
        return self.origins[p, level, other]

    def shape(self, p, level):
        return (D >> level, FC) if p < 2 else (FC // 2, D >> (level - 1))

    def window(self, ref, origin, shape):
        return ref.at[pl.ds(at(origin[0], 64), shape[0]), pl.ds(at(origin[1], 128), shape[1])]

    def landing(self, p, k, slot):
        if p < 2:
            return self.recv_gate_up[p].at[slot, pl.ds(D - (D >> k), D // 2 >> k), :]
        if k == 0:
            return self.recv_down.at[slot]
        return self.recv_down_ici.at[slot, :, pl.ds(D - (D >> (k - 1)), D >> k)]

    def halve(self, p, c, k):
        slot = lax.rem(c, RS)
        return pltpu.make_async_remote_copy(
            src_ref=self.window(self.g[p].at[slot], self.origin(p, k + 1, other=True), self.shape(p, k + 1)),
            dst_ref=self.landing(p, k, slot),
            send_sem=self.send.at[slot, p, k],
            recv_sem=self.recv.at[slot, p, k],
            device_id={"dp": self.peer(ORDER[p][k])},
        )

    def place(self, p, c, origin, shape):
        layer, start = layer_and_start(c)
        if p < 2:
            return self.out[p].at[layer, pl.ds(at(origin[0], 64), shape[0]), pl.ds(pl.multiple_of(start, 128), FC)]
        return self.out[p].at[layer, pl.ds(pl.multiple_of(start + origin[0], 16), shape[0]), pl.ds(at(origin[1], 128), shape[1])]

    def gather(self, p, c, j, q=0):
        slot, level = lax.rem(c, RS), 4 - j
        (row, column), (rows, columns) = self.origin(p, level), self.shape(p, level)
        if j == 2:
            rows = rows // 4
            row = row + q * rows
        there = self.place(p, c, (row, column), (rows, columns))
        return pltpu.make_async_remote_copy(
            src_ref=self.window(self.g[p].at[slot], (row, column), (rows, columns)) if j == 0 else there,
            dst_ref=there,
            send_sem=self.gather_send.at[c, p, 3 + q if q else j],
            recv_sem=self.gather_recv.at[c, p, 3 + q if q else j],
            device_id={"dp": self.peer(ORDER[p][3 - j])},
        )

    def keep(self, p, c, piece):
        slot = lax.rem(c, RS)
        origin, shape = self.origin(p, 4), self.shape(p, 4)
        own, sem = self.window(self.g[p].at[slot], origin, shape), self.local.at[slot, p]
        if not piece:
            return [pltpu.make_async_copy(own, self.place(p, c, origin, shape), sem)]
        there = self.pieces.at[c - NG, p]
        if p < 2:
            return [pltpu.make_async_copy(own, there, sem)]
        return [pltpu.make_async_copy(own.at[pl.ds(64 * b, 64), :], there.at[:, pl.ds(128 * b, 128)], sem) for b in range(5)]

    def kept(self, p, c):
        slot = lax.rem(c, RS)
        there = self.pieces.at[0, 0]
        return pltpu.make_async_copy(self.g[0].at[slot, pl.ds(0, D // 16), :], there, self.local.at[slot, p])

    def add(self, p, c, k):
        slot = lax.rem(c, RS)
        level = min(k + 1, 4)
        (row, column), shape = self.origin(p, level, other=k < 4), self.shape(p, level)
        ref = self.g[p]
        if p < 2:

            def block(i, carry):
                here = (slot, pl.ds(pl.multiple_of(row + i * 64, 64), 64), slice(None))
                total = ref[here].astype(F32)
                for j in range(k):
                    there = D - (D >> j) + row - self.origin(p, j + 1)[0] + i * 64
                    total = total + self.recv_gate_up[p][slot, pl.ds(pl.multiple_of(there, 64), 64), :].astype(F32)
                ref[here] = total.astype(BF)
                return carry

            lax.fori_loop(0, shape[0] // 64, block, 0)
        else:

            def block(i, carry):
                here = (slot, pl.ds(pl.multiple_of(row, 64), shape[0]), pl.ds(pl.multiple_of(column + i * 128, 128), 128))
                total = ref[here].astype(F32)
                for j in range(k):
                    there = column - self.origin(p, j + 1)[1] + i * 128
                    if j == 0:
                        total = total + self.recv_down[slot, :, pl.ds(pl.multiple_of(there, 128), 128)].astype(F32)
                    else:
                        there = there + D - (D >> (j - 1))
                        total = total + self.recv_down_ici[slot, :, pl.ds(pl.multiple_of(there, 128), 128)].astype(F32)
                ref[here] = total.astype(BF)
                return carry

            lax.fori_loop(0, shape[1] // 128, block, 0)

    def step(self, k, q, parts, c, piece):
        if k < 2:

            @pl.when(c >= RS)
            def _():
                for axis in range(1) if k == 0 else range(1, 4):
                    pl.semaphore_wait(self.free.at[axis, parts[0] // 2], 1)

        for p in parts:
            if 1 <= k <= 4:
                self.halve(p, c, k - 1).wait()
                self.add(p, c, k)
            if k < 4:
                self.halve(p, c, k).start()
            if k == 4:
                for copy in self.keep(p, c, piece):
                    copy.start()
            if k == 5:
                self.kept(p, c).wait()
            if k >= 5 and q == 0 and not piece:
                for quarter in range(4 if k == 7 else 1):
                    self.gather(p, c, k - 5, quarter).wait()
            if 4 <= k < 8 and not piece:
                self.gather(p, c, k - 4, q).start()
        if k == 4:

            @pl.when(c + RS < NC)
            def _():
                for axis, b in enumerate(AXES):
                    pl.semaphore_signal(self.free.at[axis, parts[0] // 2], inc=1, device_id={"dp": self.peer(b)})


STEPS = [(i, step) for i in range(NF) for step in range(9)] + [(i, step) for i in range(NF, NC + 8) for step in range(7)]

DIGITS = "0123456789abcdefghijklmnopqrstuvwxyzABCDEFGHIJKLMNOPQRSTUVWXYZ"
STAGES = [(k, q) for k in range(9) for q in range(4 if k == 6 else 1)]
TIMES = (
    ("57bdfimnovFK", "458cfimnpuHJ"),
    ("57bdfimnovEK", "458cfimnpuGI"),
    ("57bdfimnouEK", "458cfimnptGI"),
    ("57bdgimnuvAG", "459cegmouwFI"),
    ("568deiswwzDK", "458dejsuBBHL"),
    ("56bdfhttuvGK", "45acehpqstzH"),
    ("58cehi", "68cegh"),
    ("58cehi", "68cegh"),
    ("5agszA", "4aiqwC"),
    ("58cnxG", "46flDI"),
)


def plan():
    entries = {}
    for c, both in enumerate(TIMES):
        for parts, times in zip(((0, 1), (2,)), both, strict=True):
            for (k, q), digit in zip(STAGES, times):
                entries.setdefault(STEPS[STEPS.index((c, 0)) + DIGITS.index(digit)], []).append((k, q, parts, c))
    return entries


def first(entry):
    k, q, parts, *_ = entry
    return (k > 4, -k if k <= 4 else k, q, parts)


PLAN = plan()
LAST, FIRST = range(NF), range(NF, NC)


def backward_kernel(
    a1, a0, dy, h1, by0, hid0, wg, wu, wd,
    out_gate, out_up, out_down, pieces,
    a, by_h, by_a, wgu, wdv, hid, dgu, g_gate, g_up, g_down, recv_gate, recv_up, recv_down, recv_down_ici,
    rows_sem, load_sem, w_sem, by_sem, send, recv, gather_send, gather_recv, local, free,
):
    total = Sum(
        (g_gate, g_up, g_down), (out_gate, out_up, out_down), pieces,
        (recv_gate, recv_up), recv_down, recv_down_ici, send, recv, gather_send, gather_recv, local, free,
    )

    def weights(c, both):
        (layer, start), slot = layer_and_start(c), lax.rem(c, 2)
        columns = pl.ds(pl.multiple_of(start, 128), FC)
        copies = [pltpu.make_async_copy(wd.at[layer, pl.ds(pl.multiple_of(start, 64), FC), :], wdv.at[slot], w_sem.at[slot, 0])]
        if both:
            copies.append(pltpu.make_async_copy(wg.at[layer, :, columns], wgu.at[slot, :, pl.ds(0, FC)], w_sem.at[slot, 1]))
            copies.append(pltpu.make_async_copy(wu.at[layer, :, columns], wgu.at[slot, :, pl.ds(FC, FC)], w_sem.at[slot, 2]))
        return copies

    def rows_of(t):
        return pl.ds(pl.multiple_of(t * TB, TB), TB)

    def first_rows(t):
        return [
            pltpu.make_async_copy(dy.at[rows_of(t), :], by_h.at[rows_of(t), :], rows_sem.at[t, 0]),
            pltpu.make_async_copy(a1.at[rows_of(t), :], a.at[rows_of(t), :], rows_sem.at[t, 1]),
        ]

    def derivatives(c, t):
        return pltpu.make_async_copy(by0.at[c - NF, rows_of(t), :], by_a.at[rows_of(t), :], by_sem.at[t])

    def hidden(c):
        return pltpu.make_async_copy(hid0.at[c - NF], hid, load_sem.at[2])

    load_h1 = pltpu.make_async_copy(h1, a, load_sem.at[0])
    load_a0 = pltpu.make_async_copy(a0, a, load_sem.at[1])

    total.arrive()
    for copy in weights(0, True) + first_rows(0):
        copy.start()
    by_a[:, :D] = jnp.zeros((T, D), F32)
    total.meet()

    def sends(step, c, span):
        found = {}
        for i in span:
            for k, q, parts, chunk in PLAN.get((i, step), ()):
                found.setdefault((k, q, parts, i - chunk, chunk >= NG), []).append(i)
        runs = []
        for entry, chunks in sorted(found.items(), key=lambda e: first(e[0])):
            for low in (i for i in chunks if i - 1 not in chunks):
                high = next(i for i in chunks if i >= low and i + 1 not in chunks)
                same = [run for run in runs if run[:2] == [low, high]]
                if same and all(run[0] > high or run[1] < low for run in runs[runs.index(same[-1]) + 1 :]):
                    same[-1][2].append(entry)
                else:
                    runs.append([low, high, [entry]])
        for low, high, entries in runs:

            @pl.when(jnp.logical_and(c >= low, c <= high))
            def _(entries=entries):
                for k, q, parts, back, piece in entries:
                    total.step(k, q, parts, c - back, piece)

    def sends_of_block(t, c, span):
        for n in range(NT):

            @pl.when(t == n)
            def _(n=n):
                sends(n, c, span)

    def weight_gradients(c, span):
        slot = lax.rem(c, RS)
        g_down[slot] = dot(hid[...], by_h[...], 0, 0).astype(BF)

        @pl.when(jnp.logical_and(c >= NF - 1, c < NC - 1))
        def _():
            hidden(c + 1).start()

        sends(4, c, span)

        def block(m, carry):
            half = jnp.where(m == 0, 1 - total.core, total.core)
            rows = pl.ds(pl.multiple_of(half * (D // 2), D // 2), D // 2)
            both = dot(a[:, rows], dgu[...], 0, 0).astype(BF)
            g_gate[slot, rows, :] = both[:, :FC]
            g_up[slot, rows, :] = both[:, FC:]

            @pl.when(m == 0)
            def _():
                sends(5, c, span)

            @pl.when(m == 1)
            def _():
                sends(6, c, span)

            return carry

        lax.fori_loop(0, 2, block, 0)

    def input_rows(t, slot):
        rows = rows_of(t)
        by_a[rows, :D] += dot(dgu[rows, :], wgu[slot], 1, 1)

    def last_layer(c, carry):
        slot = lax.rem(c, 2)
        for copy in weights(c, True):
            copy.wait()

        @pl.when(jnp.logical_and(c > 0, c < NF - 1))
        def _():
            for copy in weights(c + 1, True):
                copy.start()

        @pl.when(c == NF - 1)
        def _():
            for copy in weights(c + 1, False):
                copy.start()

        def block(t, carry):
            @pl.when(c == 0)
            def _():
                for copy in first_rows(t):
                    copy.wait()

                @pl.when(t < NT - 1)
                def _():
                    for copy in first_rows(t + 1):
                        copy.start()

                @pl.when(t == NT - 1)
                def _():
                    for copy in weights(1, True):
                        copy.start()

            rows = rows_of(t)
            gu = dot(a[rows, :], wgu[slot], 1, 0)
            by_hidden = dot(by_h[rows, :], wdv[slot], 1, 1).astype(BF).astype(F32)
            hid[rows, :], by_gate, by_up = gated(gu[:, :FC], gu[:, FC:])
            dgu[rows, :FC] = (by_hidden * by_gate).astype(BF)
            dgu[rows, FC:] = (by_hidden * by_up).astype(BF)
            sends_of_block(t, c, LAST)
            return carry

        lax.fori_loop(0, NT, block, 0)

        weight_gradients(c, LAST)

        @pl.when(c == NF - 1)
        def _():
            load_h1.start()

        def input_block(t, carry):
            input_rows(t, slot)

            @pl.when(t == 1)
            def _():
                sends(7, c, LAST)

            @pl.when(t == 3)
            def _():
                sends(8, c, LAST)

            return carry

        lax.fori_loop(0, jnp.where(c < NF - 1, NT, 1), input_block, 0)
        return carry

    lax.fori_loop(0, NF, last_layer, 0)
    load_h1.wait()

    def norm_rows(t):
        for half in range(2):
            rows = pl.ds(pl.multiple_of(t * TB + half * (TB // 2), TB // 2), TB // 2)
            wide = a[rows, :].astype(F32)
            scale = inverse_rms(wide)
            by_normed = by_a[rows, :D].astype(BF).astype(F32)
            through = by_normed * scale - wide * (scale * scale * scale * jnp.mean(by_normed * wide, -1, keepdims=True))
            by_h[rows, :] = (by_h[rows, :].astype(F32) + through.astype(BF).astype(F32)).astype(BF)

    def norm_block(t, carry):
        norm_rows(t - 1)
        input_rows(t, (NF - 1) % 2)
        derivatives(NF, t - 1).start()

        @pl.when(t == 1)
        def _():
            sends(7, NF - 1, LAST[-1:])

        @pl.when(t == 3)
        def _():
            sends(8, NF - 1, LAST[-1:])

        return carry

    lax.fori_loop(1, NT, norm_block, 0)
    norm_rows(NT - 1)
    derivatives(NF, NT - 1).start()
    load_a0.start()

    def first_layer(c, carry):
        slot = lax.rem(c, 2)
        for copy in weights(c, False):
            copy.wait()

        @pl.when(c < NC - 1)
        def _():
            for copy in weights(c + 1, False):
                copy.start()

        def block(t, carry):
            rows = rows_of(t)
            derivatives(c, t).wait()
            by_hidden = dot(by_h[rows, :], wdv[slot], 1, 1).astype(BF).astype(F32)
            dgu[rows, :FC] = (by_hidden * by_a[rows, :FC]).astype(BF)
            dgu[rows, FC:] = (by_hidden * by_a[rows, FC:]).astype(BF)

            @pl.when(c < NC - 1)
            def _():
                derivatives(c + 1, t).start()

            sends_of_block(t, c, FIRST)
            return carry

        lax.fori_loop(0, NT, block, 0)
        hidden(c).wait()

        @pl.when(c == NF)
        def _():
            load_a0.wait()

        weight_gradients(c, FIRST)
        return carry

    lax.fori_loop(NF, NC, first_layer, 0)
    for (i, _), entries in sorted(PLAN.items()):
        if i >= NC:
            for k, q, parts, chunk in sorted(entries, key=first):
                total.step(k, q, parts, chunk, chunk >= NG)


def backward(a1, a0, dy, h1, by0, hid0, wg, wu, wd):
    dma = pltpu.SemaphoreType.DMA
    return pl.pallas_call(
        backward_kernel,
        out_shape=[jax.ShapeDtypeStruct(shape, BF) for shape in ((2, D, FF), (2, D, FF), (2, FF, D), (NK, 3, D // 16, FC))],
        in_specs=any_spec(9),
        out_specs=any_spec(4),
        scratch_shapes=[
            pltpu.VMEM((T, D), BF),
            pltpu.VMEM((T, D), BF),
            pltpu.VMEM((T, 2 * FC), F32),
            pltpu.VMEM((2, D, 2 * FC), BF),
            pltpu.VMEM((2, FC, D), BF),
            pltpu.VMEM((T, FC), BF),
            pltpu.VMEM((T, 2 * FC), BF),
            pltpu.VMEM((RS, D, FC), BF),
            pltpu.VMEM((RS, D, FC), BF),
            pltpu.VMEM((RS, FC, D), BF),
            pltpu.VMEM((RS, D - D // 16, FC), BF),
            pltpu.VMEM((RS, D - D // 16, FC), BF),
            pltpu.VMEM((RS, FC // 2, D), BF),
            pltpu.VMEM((RS, FC // 2, D - D // 8), BF),
            dma((NT, 2)),
            dma((3,)),
            dma((2, 3)),
            dma((NT,)),
            dma((RS, 3, 4)),
            dma((RS, 3, 4)),
            dma((NG, 3, 7)),
            dma((NG, 3, 7)),
            dma((RS, 3)),
            pltpu.SemaphoreType.REGULAR((4, 2)),
        ],
        compiler_params=pltpu.CompilerParams(collective_id=0, has_side_effects=True, vmem_limit_bytes=VMEM_LIMIT),
        cost_estimate=pl.CostEstimate(flops=24 * T * D * FF, bytes_accessed=200 * 2**20, transcendentals=2 * T * FF),
        name="backward",
    )(a1, a0, dy, h1, by0, hid0, wg, wu, wd)


SLOTS = 4
QUARTERS = ((D // 4, FC), (D // 4, FC), (FC // 4, D))


def adamw(w, m, v, g):
    m = 0.9 * m + 0.1 * g
    v = 0.95 * v + 0.05 * g * g
    step = m * lax.rsqrt(v + 1e-8) + 0.1 * w
    return (w - 0.02 * step).astype(BF), m, v


def owner(p, half, q):
    bits = ORDER[p]
    return half * bits[0] + q // 4 * bits[1] + q // 2 % 2 * bits[2] + q % 2 * bits[3]


def adamw_kernel(chunks, in_pieces, n_before, *refs):
    w, m, v = refs[0:3], refs[3:6], refs[6:9]
    n_g = 1 if in_pieces else 3
    g, outs = refs[9 : 9 + n_g], refs[9 + n_g + n_before : 18 + n_g + n_before]
    *bufs, load_sem, store_sem = refs[18 + n_g + n_before :]
    units = 4 * len(chunks)

    def window(ref, p, c, q):
        rows, columns = QUARTERS[p]
        layer, start = layer_and_start(c)
        if p < 2:
            return ref.at[layer, pl.ds(pl.multiple_of(q * rows, rows), rows), pl.ds(pl.multiple_of(start, 128), FC)]
        return ref.at[layer, pl.ds(pl.multiple_of(start + q * rows, 32), rows), :]

    def gradient(p, c, q, to, sem):
        if not in_pieces:
            return [pltpu.make_async_copy(window(g[p], p, c, q), to, sem)]
        half, low = split(q, 2)
        if p < 2:
            return [
                pltpu.make_async_copy(g[0].at[owner(p, half, e) + low * ORDER[p][1], c - NG, p], to.at[pl.ds(64 * e, 64), :], sem) for e in range(4)
            ]
        copies = []
        for e in range(8):
            piece, columns = g[0].at[owner(p, half, e), c - NG, p], pl.ds(128 * e, 128)
            for b, rows, src, dst in ((3 * low, 64, 0, 32 * low), (1 + 3 * low, 64, 0, 64 + 32 * low), (2, 32, 32 * low, 128 - 128 * low)):
                there = pl.ds(pl.multiple_of(128 * b, 128), 128)
                copies.append(
                    pltpu.make_async_copy(
                        piece.at[pl.ds(at(src, 32), rows), there], to.at[pl.ds(pl.multiple_of(dst, 32), rows), columns], sem
                    )
                )
        return copies

    def loads(n, act):
        (c, q), slot = split(n + 4 * chunks[0], 4), lax.rem(n, SLOTS)
        for p in range(3):
            for b, ref in enumerate((w[p], m[p], v[p])):
                copy = pltpu.make_async_copy(window(ref, p, c, q), bufs[4 * p + b].at[slot], load_sem.at[slot, p, b])
                copy.start() if act == "start" else copy.wait()
            to, sem = bufs[4 * p + 3].at[slot], load_sem.at[slot, p, 3]
            if act == "start":
                for copy in gradient(p, c, q, to, sem):
                    copy.start()
            else:
                pltpu.make_async_copy(window(w[p], p, c, q), to, sem).wait()

    def stores(n, act):
        (c, q), slot = split(n + 4 * chunks[0], 4), lax.rem(n, SLOTS)
        for p in range(3):
            for b in range(3):
                copy = pltpu.make_async_copy(bufs[4 * p + b].at[slot], window(outs[3 * b + p], p, c, q), store_sem.at[slot, p, b])
                copy.start() if act == "start" else copy.wait()

    loads(0, "start")
    loads(1, "start")

    def unit(n, carry):
        slot = lax.rem(n, SLOTS)

        @pl.when(n >= 2)
        def _():
            stores(n - 2, "wait")

        @pl.when(n + 2 < units)
        def _():
            loads(n + 2, "start")

        loads(n, "wait")
        for p in range(3):
            block = 64 if p < 2 else 32

            def rows_block(r, carry, buf=bufs[4 * p : 4 * p + 4], block=block):
                here = (slot, pl.ds(pl.multiple_of(r * block, block), block), slice(None))
                buf[0][here], buf[1][here], buf[2][here] = adamw(
                    buf[0][here].astype(F32), buf[1][here], buf[2][here], buf[3][here].astype(F32)
                )
                return carry

            lax.fori_loop(0, QUARTERS[p][0] // block, rows_block, 0)
        stores(n, "start")
        return carry

    lax.fori_loop(0, units, unit, 0)
    stores(units - 2, "wait")
    stores(units - 1, "wait")


def adamw_call(chunks, arrays, gradients, before=()):
    in_pieces, n_before = len(gradients) == 1, len(before)

    def kernel(*refs):
        adamw_kernel(chunks, in_pieces, n_before, *refs)

    elements, n_in = 3 * D * FC * len(chunks), 9 + len(gradients)
    return pl.pallas_call(
        kernel,
        out_shape=[jax.ShapeDtypeStruct(a.shape, a.dtype) for a in arrays],
        in_specs=any_spec(n_in + n_before),
        out_specs=any_spec(9),
        input_output_aliases={n_in + i: i for i in range(n_before)},
        scratch_shapes=[pltpu.VMEM((SLOTS, *shape), t) for shape in QUARTERS for t in (BF, F32, F32, BF)]
        + [pltpu.SemaphoreType.DMA((SLOTS, 3, 4)), pltpu.SemaphoreType.DMA((SLOTS, 3, 3))],
        compiler_params=pltpu.CompilerParams(vmem_limit_bytes=VMEM_LIMIT),
        cost_estimate=pl.CostEstimate(flops=15 * elements, bytes_accessed=22 * elements, transcendentals=elements),
        name="adamw_pieces" if in_pieces else "adamw_whole",
    )(*arrays, *gradients, *before)


def solution(mesh):
    def step(x, dy, *arrays):
        weights = arrays[:3]
        by0, hid0, h1, a1, a0 = forward(x[0], *weights)
        *gradients, pieces = backward(a1, a0, dy[0], h1, by0, hid0, *weights)
        gathered = lax.all_gather(pieces, "dp")
        new = adamw_call(range(NG), arrays, gradients)
        return tuple(adamw_call(range(NG, NC), arrays, (gathered,), new))

    return jax.shard_map(
        step,
        mesh=mesh,
        in_specs=(P(("rep", "dp"), None, None),) * 2 + (P(None, None, None),) * 9,
        out_specs=(P("rep", None, None),) * 9,
        check_vma=False,
    )
```

```python
import jax
import jax.numpy as jnp
from jax import lax
from jax.experimental import pallas as pl
from jax.experimental.pallas import tpu as pltpu
from jax.sharding import PartitionSpec as P

BF, F32 = jnp.bfloat16, jnp.float32
T, D, FF = 2048, 1024, 3200
FC = 640
NF = FF // FC
NC = 2 * NF
TB = 512
NT = T // TB
NG = NF + 1
NK = NC - NG
BETWEEN = -1
RS = 2
VMEM_LIMIT = 63 << 20

AXES = (1, 8, 4, 2)
ORDER = (AXES, (1, 4, 2, 8), (1, 2, 8, 4))


def dot(a, b, ca, cb):
    return lax.dot_general(a, b, (((ca,), (cb,)), ((), ())), preferred_element_type=F32)


def inverse_rms(wide):
    return lax.rsqrt(jnp.mean(wide * wide, -1, keepdims=True) + 1e-6)


def gated(gate, up):
    s = 1.0 / (1.0 + jnp.exp(-gate))
    silu = gate * s
    return (silu * up).astype(BF), up * (s + silu * (1.0 - s)), silu


def split(a, b):
    return (a // b, a % b) if isinstance(a, int) else (lax.div(a, jnp.int32(b)), lax.rem(a, jnp.int32(b)))


def layer_and_start(c):
    before, chunk = split(c, NF)
    return 1 - before, chunk * FC


def any_spec(n):
    return [pl.BlockSpec(memory_space=pl.ANY)] * n


def forward_kernel(x_ref, wg, wu, wd, by0, hid0, h1_ref, a1_ref, a0_ref, wgu, wdv, hid, byb, wsem, dsem, osem, hsem):
    i = pl.program_id(0)
    rows = pl.ds(pl.multiple_of(i * TB, TB), TB)

    def columns(c):
        return pl.ds(pl.multiple_of(c * FC, 128), FC)

    def weights(c):
        return (
            pltpu.make_async_copy(wg.at[0, :, columns(c)], wgu.at[c, :, pl.ds(0, FC)], wsem.at[c, 0]),
            pltpu.make_async_copy(wu.at[0, :, columns(c)], wgu.at[c, :, pl.ds(FC, FC)], wsem.at[c, 1]),
        )

    down = pltpu.make_async_copy(wd.at[0], wdv, dsem)

    @pl.when(i == 0)
    def _():
        for c in range(NF):
            for copy in weights(c):
                copy.start()
        down.start()

    def out_by(c):
        return pltpu.make_async_copy(byb.at[lax.rem(c, 2)], by0.at[c, rows, :], osem.at[lax.rem(c, 2)])

    def out_hid(c):
        return pltpu.make_async_copy(hid.at[:, columns(c)], hid0.at[c, rows, :], hsem.at[c])

    wide = x_ref[...].astype(F32)
    a0_ref[...] = (wide * inverse_rms(wide)).astype(BF)

    def chunk(c, carry):
        @pl.when(i == 0)
        def _():
            for copy in weights(c):
                copy.wait()

        @pl.when(c >= 2)
        def _():
            out_by(c).wait()

        gu = dot(a0_ref[...], wgu[c], 1, 0)
        hid[:, columns(c)], byb[lax.rem(c, 2), :, :FC], byb[lax.rem(c, 2), :, FC:] = gated(gu[:, :FC], gu[:, FC:])
        out_by(c).start()
        out_hid(c).start()
        return carry

    lax.fori_loop(0, NF, chunk, 0)

    @pl.when(i == 0)
    def _():
        down.wait()

    h1_ref[...] = (x_ref[...].astype(F32) + dot(hid[...], wdv[...], 1, 0).astype(BF).astype(F32)).astype(BF)
    wide1 = h1_ref[...].astype(F32)
    a1_ref[...] = (wide1 * inverse_rms(wide1)).astype(BF)
    for c in range(NF):
        out_hid(c).wait()
    out_by(NF - 2).wait()
    out_by(NF - 1).wait()


def forward(x, wg, wu, wd):
    rows = pl.BlockSpec((TB, D), lambda i: (i, 0))
    dma = pltpu.SemaphoreType.DMA
    return pl.pallas_call(
        forward_kernel,
        grid=(NT,),
        out_shape=[
            jax.ShapeDtypeStruct((NF, T, 2 * FC), F32),
            jax.ShapeDtypeStruct((NF, T, FC), BF),
            jax.ShapeDtypeStruct((T, D), BF),
            jax.ShapeDtypeStruct((T, D), BF),
            jax.ShapeDtypeStruct((T, D), BF),
        ],
        in_specs=[rows] + any_spec(3),
        out_specs=any_spec(2) + [rows] * 3,
        scratch_shapes=[
            pltpu.VMEM((NF, D, 2 * FC), BF),
            pltpu.VMEM((FF, D), BF),
            pltpu.VMEM((TB, FF), BF),
            pltpu.VMEM((2, TB, 2 * FC), F32),
            dma((NF, 2)),
            dma,
            dma((2,)),
            dma((NF,)),
        ],
        compiler_params=pltpu.CompilerParams(dimension_semantics=("arbitrary",), vmem_limit_bytes=VMEM_LIMIT),
        cost_estimate=pl.CostEstimate(flops=6 * T * D * FF, bytes_accessed=110 << 20, transcendentals=T * FF),
        name="forward",
    )(x, wg, wu, wd)


def at(x, m):
    return x if isinstance(x, int) else pl.multiple_of(x, m)


class Sum:
    def __init__(self, g, out, pieces, recv_gate_up, recv_down, recv_down_ici, send, recv, gather_send, gather_recv, local, free):
        self.g, self.out, self.pieces = g, out, pieces
        self.recv_gate_up, self.recv_down, self.recv_down_ici = recv_gate_up, recv_down, recv_down_ici
        self.send, self.recv, self.local, self.free = send, recv, local, free
        self.gather_send, self.gather_recv = gather_send, gather_recv
        me = lax.axis_index("dp")
        bits = {b: split(split(me, b)[0], 2)[1] for b in AXES}
        self.core = bits[1]
        self.peers = {b: me + b * (1 - 2 * bits[b]) for b in AXES}
        self.origins = {}
        for p in range(3):
            row = column = 0
            self.origins[p, 0, False] = row, column
            for k, b in enumerate(ORDER[p]):
                for other in (True, False):
                    h = 1 - bits[b] if other else bits[b]
                    if p < 2:
                        here = row + h * (D // 2 >> k), column
                    elif k == 0:
                        here = row + h * (FC // 2), column
                    else:
                        here = row, column + h * (D >> k)
                    self.origins[p, k + 1, other] = here
                row, column = here

    def peer(self, b):
        return self.peers[b]

    def arrive(self):
        for b in AXES:
            pl.semaphore_signal(pltpu.get_barrier_semaphore(), inc=1, device_id={"dp": self.peer(b)})

    def meet(self):
        pl.semaphore_wait(pltpu.get_barrier_semaphore(), len(AXES))

    def origin(self, p, level, other=False):
        return self.origins[p, level, other]

    def shape(self, p, level):
        return (D >> level, FC) if p < 2 else (FC // 2, D >> (level - 1))

    def window(self, ref, origin, shape):
        return ref.at[pl.ds(at(origin[0], 64), shape[0]), pl.ds(at(origin[1], 128), shape[1])]

    def landing(self, p, k, slot):
        if p < 2:
            return self.recv_gate_up[p].at[slot, pl.ds(D - (D >> k), D // 2 >> k), :]
        if k == 0:
            return self.recv_down.at[slot]
        return self.recv_down_ici.at[slot, :, pl.ds(D - (D >> (k - 1)), D >> k)]

    def halve(self, p, c, k):
        slot = lax.rem(c, RS)
        return pltpu.make_async_remote_copy(
            src_ref=self.window(self.g[p].at[slot], self.origin(p, k + 1, other=True), self.shape(p, k + 1)),
            dst_ref=self.landing(p, k, slot),
            send_sem=self.send.at[slot, p, k],
            recv_sem=self.recv.at[slot, p, k],
            device_id={"dp": self.peer(ORDER[p][k])},
        )

    def place(self, p, c, origin, shape):
        layer, start = layer_and_start(c)
        if p < 2:
            return self.out[p].at[layer, pl.ds(at(origin[0], 64), shape[0]), pl.ds(pl.multiple_of(start, 128), FC)]
        return self.out[p].at[layer, pl.ds(pl.multiple_of(start + origin[0], 16), shape[0]), pl.ds(at(origin[1], 128), shape[1])]

    def gather(self, p, c, j, q=0):
        slot, level = lax.rem(c, RS), 4 - j
        (row, column), (rows, columns) = self.origin(p, level), self.shape(p, level)
        if j == 2:
            rows = rows // 4
            row = row + q * rows
        there = self.place(p, c, (row, column), (rows, columns))
        return pltpu.make_async_remote_copy(
            src_ref=self.window(self.g[p].at[slot], (row, column), (rows, columns)) if j == 0 else there,
            dst_ref=there,
            send_sem=self.gather_send.at[c, p, 3 + q if q else j],
            recv_sem=self.gather_recv.at[c, p, 3 + q if q else j],
            device_id={"dp": self.peer(ORDER[p][3 - j])},
        )

    def keep(self, p, c, piece):
        slot = lax.rem(c, RS)
        origin, shape = self.origin(p, 4), self.shape(p, 4)
        own, sem = self.window(self.g[p].at[slot], origin, shape), self.local.at[slot, p]
        if not piece:
            return [pltpu.make_async_copy(own, self.place(p, c, origin, shape), sem)]
        there = self.pieces.at[c - NG, p]
        if p < 2:
            return [pltpu.make_async_copy(own, there, sem)]
        return [pltpu.make_async_copy(own.at[pl.ds(64 * b, 64), :], there.at[:, pl.ds(128 * b, 128)], sem) for b in range(5)]

    def kept(self, p, c):
        slot = lax.rem(c, RS)
        there = self.pieces.at[0, 0]
        return pltpu.make_async_copy(self.g[0].at[slot, pl.ds(0, D // 16), :], there, self.local.at[slot, p])

    def add(self, p, c, k):
        slot = lax.rem(c, RS)
        level = min(k + 1, 4)
        (row, column), shape = self.origin(p, level, other=k < 4), self.shape(p, level)
        ref = self.g[p]
        if p < 2:

            def block(i, carry):
                here = (slot, pl.ds(pl.multiple_of(row + i * 64, 64), 64), slice(None))
                total = ref[here].astype(F32)
                for j in range(k):
                    there = D - (D >> j) + row - self.origin(p, j + 1)[0] + i * 64
                    total = total + self.recv_gate_up[p][slot, pl.ds(pl.multiple_of(there, 64), 64), :].astype(F32)
                ref[here] = total.astype(BF)
                return carry

            lax.fori_loop(0, shape[0] // 64, block, 0)
        else:

            def block(i, carry):
                here = (slot, pl.ds(pl.multiple_of(row, 64), shape[0]), pl.ds(pl.multiple_of(column + i * 128, 128), 128))
                total = ref[here].astype(F32)
                for j in range(k):
                    there = column - self.origin(p, j + 1)[1] + i * 128
                    if j == 0:
                        total = total + self.recv_down[slot, :, pl.ds(pl.multiple_of(there, 128), 128)].astype(F32)
                    else:
                        there = there + D - (D >> (j - 1))
                        total = total + self.recv_down_ici[slot, :, pl.ds(pl.multiple_of(there, 128), 128)].astype(F32)
                ref[here] = total.astype(BF)
                return carry

            lax.fori_loop(0, shape[1] // 128, block, 0)

    def step(self, k, q, parts, c, piece):
        group = parts[0] // 2
        if k < 2:

            @pl.when(c >= RS)
            def _():
                for axis in range(1) if k == 0 else range(1, 4):
                    pl.semaphore_wait(self.free.at[axis, group], 1)

        for p in parts:
            if 1 <= k <= 4:
                self.halve(p, c, k - 1).wait()
                self.add(p, c, k)
            if k < 4:
                self.halve(p, c, k).start()
            if k == 4:
                for copy in self.keep(p, c, piece):
                    copy.start()
            if k == 5:
                self.kept(p, c).wait()
            if k >= 5 and q == 0 and not piece:
                for quarter in range(4 if k == 7 else 1):
                    self.gather(p, c, k - 5, quarter).wait()
            if 4 <= k < 8 and not piece:
                self.gather(p, c, k - 4, q).start()
        if k == 4:

            @pl.when(c + RS < NC)
            def _():
                for axis, b in enumerate(AXES):
                    pl.semaphore_signal(self.free.at[axis, group], inc=1, device_id={"dp": self.peer(b)})


STEPS = [(i, step) for i in range(NF) for step in range(7)] + [(BETWEEN, step) for step in range(10)]
STEPS += [(i, step) for i in range(NF, NC + 8) for step in range(7)]

DIGITS = "0123456789abcdefghijklmnopqrstuvwxyzABCDEFGHIJKLMNOPQRSTUVWXYZ"
STAGES = [(k, q) for k in range(9) for q in range(4 if k == 6 else 1)]
TIMES = (
    ("57bdgirDFJUX", "46acehkvvJRX"),
    ("56adginrvBIM", "45acehrtvwJP"),
    ("56adginrvAIM", "45acehrtvvJP"),
    ("57bdgmootzBQ", "45adglnotOSX"),
    ("57adekrtyJRW", "46aefgmstyOX"),
    ("56bcfinrttCE", "46bcdhmsvxBH"),
    ("56behi", "45adgh"),
    ("58cegi", "48cegh"),
    ("58gouA", "57gsxF"),
    ("58bmCV", "47bmFW"),
)


def plan():
    entries = {}
    for c, both in enumerate(TIMES):
        for parts, times in zip(((0, 1), (2,)), both, strict=True):
            for (k, q), digit in zip(STAGES, times):
                entries.setdefault(STEPS[STEPS.index((c, 0)) + DIGITS.index(digit)], []).append((k, q, parts, c))
    return entries


def first(entry):
    k, q, parts, *_ = entry
    return (k > 4, -k if k <= 4 else k, q, parts)


PLAN = plan()
LAST, FIRST = range(NF), range(NF, NC)


def backward_kernel(
    a1, a0, dy, h1, by0, hid0, wg, wu, wd,
    out_gate, out_up, out_down, pieces, kept_dgu,
    a, by_h, by_a, wgu, wdv, hid, dgu, g_gate, g_up, g_down, recv_gate, recv_up, recv_down, recv_down_ici,
    rows_sem, load_sem, w_sem, by_sem, dgu_sem, send, recv, gather_send, gather_recv, local, free,
):
    total = Sum(
        (g_gate, g_up, g_down), (out_gate, out_up, out_down), pieces,
        (recv_gate, recv_up), recv_down, recv_down_ici, send, recv, gather_send, gather_recv, local, free,
    )

    def down_weights(c):
        (layer, start), slot = layer_and_start(c), lax.rem(c, 2)
        return [pltpu.make_async_copy(wd.at[layer, pl.ds(pl.multiple_of(start, 64), FC), :], wdv.at[slot], w_sem.at[slot, 2])]

    def input_weights(c):
        (layer, start), slot = layer_and_start(c), lax.rem(c, 2)
        columns = pl.ds(pl.multiple_of(start, 128), FC)
        return [
            pltpu.make_async_copy(w.at[layer, :, columns], wgu.at[slot, :, pl.ds(i * FC, FC)], w_sem.at[slot, i]) for i, w in enumerate((wg, wu))
        ]

    def rows_of(t):
        return pl.ds(pl.multiple_of(t * TB, TB), TB)

    def first_rows(t):
        return [
            pltpu.make_async_copy(dy.at[rows_of(t), :], by_h.at[rows_of(t), :], rows_sem.at[t, 0]),
            pltpu.make_async_copy(a1.at[rows_of(t), :], a.at[rows_of(t), :], rows_sem.at[t, 1]),
        ]

    def derivatives(c, t):
        return pltpu.make_async_copy(by0.at[c - NF, rows_of(t), :], by_a.at[rows_of(t), :], by_sem.at[t])

    def keep_dgu(c, t):
        return pltpu.make_async_copy(dgu.at[rows_of(t), :], kept_dgu.at[c, rows_of(t), :], dgu_sem.at[t])

    def fetch_dgu(c, t):
        return pltpu.make_async_copy(kept_dgu.at[c, rows_of(t), :], dgu.at[rows_of(t), :], dgu_sem.at[t])

    def hidden(c):
        return pltpu.make_async_copy(hid0.at[c - NF], hid, load_sem.at[2])

    load_h1 = pltpu.make_async_copy(h1, a, load_sem.at[0])
    load_a0 = pltpu.make_async_copy(a0, a, load_sem.at[1])

    total.arrive()
    for copy in down_weights(0) + input_weights(0) + first_rows(0):
        copy.start()
    by_a[:, :D] = jnp.zeros((T, D), F32)
    total.meet()

    def sends(step, c, span):
        found = {}
        for i in span:
            for k, q, parts, chunk in PLAN.get((i, step), ()):
                found.setdefault((k, q, parts, i - chunk, chunk >= NG), []).append(i)
        runs = []
        for entry, chunks in sorted(found.items(), key=lambda e: first(e[0])):
            for low in (i for i in chunks if i - 1 not in chunks):
                high = next(i for i in chunks if i >= low and i + 1 not in chunks)
                same = [run for run in runs if run[:2] == [low, high]]
                if same and all(run[0] > high or run[1] < low for run in runs[runs.index(same[-1]) + 1 :]):
                    same[-1][2].append(entry)
                else:
                    runs.append([low, high, [entry]])
        for low, high, entries in runs:

            @pl.when(jnp.logical_and(c >= low, c <= high))
            def _(entries=entries):
                for k, q, parts, back, piece in entries:
                    total.step(k, q, parts, c - back, piece)

    def sends_of_block(t, c, span):
        for n in range(NT):

            @pl.when(t == n)
            def _(n=n):
                sends(n, c, span)

    def weight_gradients(c, span):
        slot = lax.rem(c, RS)
        g_down[slot] = dot(hid[...], by_h[...], 0, 0).astype(BF)

        @pl.when(jnp.logical_and(c >= NF - 1, c < NC - 1))
        def _():
            hidden(c + 1).start()

        sends(4, c, span)

        def block(m, carry):
            half = jnp.where(m == 0, 1 - total.core, total.core)
            rows = pl.ds(pl.multiple_of(half * (D // 2), D // 2), D // 2)
            both = dot(a[:, rows], dgu[...], 0, 0).astype(BF)
            g_gate[slot, rows, :] = both[:, :FC]
            g_up[slot, rows, :] = both[:, FC:]

            @pl.when(m == 0)
            def _():
                sends(5, c, span)

            @pl.when(m == 1)
            def _():
                sends(6, c, span)

            return carry

        lax.fori_loop(0, 2, block, 0)

    def input_rows(t, slot):
        rows = rows_of(t)
        by_a[rows, :D] += dot(dgu[rows, :], wgu[slot], 1, 1)

    def last_layer(c, carry):
        slot = lax.rem(c, 2)
        for copy in down_weights(c) + input_weights(c):
            copy.wait()

        @pl.when(jnp.logical_and(c > 0, c < NF - 1))
        def _():
            for copy in down_weights(c + 1) + input_weights(c + 1):
                copy.start()

        @pl.when(c == NF - 1)
        def _():
            for copy in down_weights(c + 1):
                copy.start()

        def block(t, carry):
            @pl.when(c == 0)
            def _():
                for copy in first_rows(t):
                    copy.wait()

                @pl.when(t < NT - 1)
                def _():
                    for copy in first_rows(t + 1):
                        copy.start()

                @pl.when(t == NT - 1)
                def _():
                    for copy in down_weights(1) + input_weights(1):
                        copy.start()

            @pl.when(c > 0)
            def _():
                keep_dgu(c - 1, t).wait()

            rows = rows_of(t)
            gu = dot(a[rows, :], wgu[slot], 1, 0)
            by_hidden = dot(by_h[rows, :], wdv[slot], 1, 1).astype(BF).astype(F32)
            hid[rows, :], by_gate, by_up = gated(gu[:, :FC], gu[:, FC:])
            dgu[rows, :FC] = (by_hidden * by_gate).astype(BF)
            dgu[rows, FC:] = (by_hidden * by_up).astype(BF)

            @pl.when(c < NF - 1)
            def _():
                keep_dgu(c, t).start()

            sends_of_block(t, c, LAST)
            return carry

        lax.fori_loop(0, NT, block, 0)

        weight_gradients(c, LAST)

        return carry

    lax.fori_loop(0, NF, last_layer, 0)
    load_h1.start()

    def sends_between(step):
        for n in range(10):
            if (BETWEEN, n) in PLAN:

                @pl.when(step == n)
                def _(n=n):
                    for k, q, parts, chunk in sorted(PLAN[BETWEEN, n], key=first):
                        total.step(k, q, parts, chunk, chunk >= NG)

    def input_chunk(n, carry):
        c = NF - 1 - n
        slot = lax.rem(c, 2)

        @pl.when(n >= 2)
        def _():
            for copy in input_weights(c):
                copy.wait()

        @pl.when(jnp.logical_and(n >= 1, c > 0))
        def _():
            for copy in input_weights(c - 1):
                copy.start()

        def input_block(t, carry):
            @pl.when(n >= 1)
            def _():
                fetch_dgu(c, t).wait()

            input_rows(t, slot)

            @pl.when(c > 0)
            def _():
                fetch_dgu(c - 1, t).start()

            pair, odd = split(t, 2)

            @pl.when(odd == 1)
            def _():
                sends_between(2 * n + pair)

            return carry

        lax.fori_loop(0, jnp.where(c > 0, NT, 1), input_block, 0)
        return carry

    lax.fori_loop(0, NF, input_chunk, 0)
    load_h1.wait()

    def norm_rows(t):
        for half in range(2):
            rows = pl.ds(pl.multiple_of(t * TB + half * (TB // 2), TB // 2), TB // 2)
            wide = a[rows, :].astype(F32)
            scale = inverse_rms(wide)
            by_normed = by_a[rows, :D].astype(BF).astype(F32)
            through = by_normed * scale - wide * (scale * scale * scale * jnp.mean(by_normed * wide, -1, keepdims=True))
            by_h[rows, :] = (by_h[rows, :].astype(F32) + through.astype(BF).astype(F32)).astype(BF)

    def norm_block(t, carry):
        fetch_dgu(0, t).wait()
        norm_rows(t - 1)
        input_rows(t, 0)
        derivatives(NF, t - 1).start()

        pair, odd = split(t, 2)

        @pl.when(odd == 1)
        def _():
            sends_between(2 * (NF - 1) + pair)

        return carry

    lax.fori_loop(1, NT, norm_block, 0)
    norm_rows(NT - 1)
    derivatives(NF, NT - 1).start()
    load_a0.start()

    def first_layer(c, carry):
        slot = lax.rem(c, 2)
        for copy in down_weights(c):
            copy.wait()

        @pl.when(c < NC - 1)
        def _():
            for copy in down_weights(c + 1):
                copy.start()

        def block(t, carry):
            rows = rows_of(t)
            derivatives(c, t).wait()
            by_hidden = dot(by_h[rows, :], wdv[slot], 1, 1).astype(BF).astype(F32)
            dgu[rows, :FC] = (by_hidden * by_a[rows, :FC]).astype(BF)
            dgu[rows, FC:] = (by_hidden * by_a[rows, FC:]).astype(BF)

            @pl.when(c < NC - 1)
            def _():
                derivatives(c + 1, t).start()

            sends_of_block(t, c, FIRST)
            return carry

        lax.fori_loop(0, NT, block, 0)
        hidden(c).wait()

        @pl.when(c == NF)
        def _():
            load_a0.wait()

        weight_gradients(c, FIRST)
        return carry

    lax.fori_loop(NF, NC, first_layer, 0)
    for (i, _), entries in sorted(PLAN.items()):
        if i >= NC:
            for k, q, parts, chunk in sorted(entries, key=first):
                total.step(k, q, parts, chunk, chunk >= NG)


def backward(a1, a0, dy, h1, by0, hid0, wg, wu, wd):
    dma = pltpu.SemaphoreType.DMA
    return pl.pallas_call(
        backward_kernel,
        out_shape=[jax.ShapeDtypeStruct(shape, BF) for shape in ((2, D, FF), (2, D, FF), (2, FF, D), (NK, 3, D // 16, FC), (NF - 1, T, 2 * FC))],
        in_specs=any_spec(9),
        out_specs=any_spec(5),
        scratch_shapes=[
            pltpu.VMEM((T, D), BF),
            pltpu.VMEM((T, D), BF),
            pltpu.VMEM((T, 2 * FC), F32),
            pltpu.VMEM((2, D, 2 * FC), BF),
            pltpu.VMEM((2, FC, D), BF),
            pltpu.VMEM((T, FC), BF),
            pltpu.VMEM((T, 2 * FC), BF),
            pltpu.VMEM((RS, D, FC), BF),
            pltpu.VMEM((RS, D, FC), BF),
            pltpu.VMEM((RS, FC, D), BF),
            pltpu.VMEM((RS, D - D // 16, FC), BF),
            pltpu.VMEM((RS, D - D // 16, FC), BF),
            pltpu.VMEM((RS, FC // 2, D), BF),
            pltpu.VMEM((RS, FC // 2, D - D // 8), BF),
            dma((NT, 2)),
            dma((3,)),
            dma((2, 3)),
            dma((NT,)),
            dma((NT,)),
            dma((RS, 3, 4)),
            dma((RS, 3, 4)),
            dma((NG, 3, 7)),
            dma((NG, 3, 7)),
            dma((RS, 3)),
            pltpu.SemaphoreType.REGULAR((4, 2)),
        ],
        compiler_params=pltpu.CompilerParams(collective_id=0, has_side_effects=True, vmem_limit_bytes=VMEM_LIMIT),
        cost_estimate=pl.CostEstimate(flops=24 * T * D * FF, bytes_accessed=200 << 20, transcendentals=2 * T * FF),
        name="backward",
    )(a1, a0, dy, h1, by0, hid0, wg, wu, wd)


SLOTS = 4
HALVES = ((D // 2, FC), (D // 2, FC), (FC // 2, D))


def adamw(w, m, v, g):
    m = 0.9 * m + 0.1 * g
    v = 0.95 * v + 0.05 * g * g
    step = m * lax.rsqrt(v + 1e-8) + 0.1 * w
    return (w - 0.02 * step).astype(BF), m, v


def owner(p, half, q):
    bits = ORDER[p]
    return half * bits[0] + q // 4 * bits[1] + q // 2 % 2 * bits[2] + q % 2 * bits[3]


def adamw_kernel(chunks, in_pieces, n_before, *refs):
    w, m, v = refs[0:3], refs[3:6], refs[6:9]
    n_g = 1 if in_pieces else 3
    g, outs = refs[9 : 9 + n_g], refs[9 + n_g + n_before : 18 + n_g + n_before]
    *bufs, load_sem, store_sem = refs[18 + n_g + n_before :]
    units, units_before = 2 * len(chunks), 2 * chunks[0]

    def window(ref, p, c, half):
        rows, columns = HALVES[p]
        layer, start = layer_and_start(c)
        if p < 2:
            return ref.at[layer, pl.ds(pl.multiple_of(half * rows, rows), rows), pl.ds(pl.multiple_of(start, 128), FC)]
        return ref.at[layer, pl.ds(pl.multiple_of(start + half * rows, 64), rows), :]

    def gradient(p, c, half, to, sem):
        if not in_pieces:
            return [pltpu.make_async_copy(window(g[p], p, c, half), to, sem)]
        copies = []
        for e in range(8):
            piece = g[0].at[owner(p, half, e), c - NG, p]
            if p < 2:
                copies.append(pltpu.make_async_copy(piece, to.at[pl.ds(64 * e, 64), :], sem))
            else:
                for b in range(5):
                    there = to.at[pl.ds(64 * b, 64), pl.ds(128 * e, 128)]
                    copies.append(pltpu.make_async_copy(piece.at[:, pl.ds(128 * b, 128)], there, sem))
        return copies

    def loads(n, act):
        (c, half), slot = split(n + units_before, 2), lax.rem(n, SLOTS)
        for p in range(3):
            for b, ref in enumerate((w[p], m[p], v[p])):
                copy = pltpu.make_async_copy(window(ref, p, c, half), bufs[4 * p + b].at[slot], load_sem.at[slot, p, b])
                copy.start() if act == "start" else copy.wait()
            to, sem = bufs[4 * p + 3].at[slot], load_sem.at[slot, p, 3]
            if act == "start":
                for copy in gradient(p, c, half, to, sem):
                    copy.start()
            else:
                pltpu.make_async_copy(window(w[p], p, c, half), to, sem).wait()

    def stores(n, act):
        (c, half), slot = split(n + units_before, 2), lax.rem(n, SLOTS)
        for p in range(3):
            for b in range(3):
                copy = pltpu.make_async_copy(bufs[4 * p + b].at[slot], window(outs[3 * b + p], p, c, half), store_sem.at[slot, p, b])
                copy.start() if act == "start" else copy.wait()

    loads(0, "start")
    loads(1, "start")

    def unit(n, carry):
        slot = lax.rem(n, SLOTS)

        @pl.when(n >= 2)
        def _():
            stores(n - 2, "wait")

        loads(n, "wait")

        @pl.when(n + 2 < units)
        def _():
            loads(n + 2, "start")

        for p in range(3):
            block = 64 if p < 2 else 32

            def rows_block(r, carry, buf=bufs[4 * p : 4 * p + 4], block=block):
                here = (slot, pl.ds(pl.multiple_of(r * block, block), block), slice(None))
                buf[0][here], buf[1][here], buf[2][here] = adamw(
                    buf[0][here].astype(F32), buf[1][here], buf[2][here], buf[3][here].astype(F32)
                )
                return carry

            lax.fori_loop(0, HALVES[p][0] // block, rows_block, 0)
        stores(n, "start")
        return carry

    lax.fori_loop(0, units, unit, 0)
    stores(units - 2, "wait")
    stores(units - 1, "wait")


def adamw_call(chunks, arrays, gradients, before=()):
    in_pieces, n_before = len(gradients) == 1, len(before)

    def kernel(*refs):
        adamw_kernel(chunks, in_pieces, n_before, *refs)

    elements, n_in = 3 * D * FC * len(chunks), 9 + len(gradients)
    return pl.pallas_call(
        kernel,
        out_shape=[jax.ShapeDtypeStruct(a.shape, a.dtype) for a in arrays],
        in_specs=any_spec(n_in + n_before),
        out_specs=any_spec(9),
        input_output_aliases={n_in + i: i for i in range(n_before)},
        scratch_shapes=[pltpu.VMEM((SLOTS, *shape), t) for shape in HALVES for t in (BF, F32, F32, BF)]
        + [pltpu.SemaphoreType.DMA((SLOTS, 3, 4)), pltpu.SemaphoreType.DMA((SLOTS, 3, 3))],
        compiler_params=pltpu.CompilerParams(vmem_limit_bytes=VMEM_LIMIT),
        cost_estimate=pl.CostEstimate(flops=15 * elements, bytes_accessed=22 * elements, transcendentals=elements),
        name="adamw_pieces" if in_pieces else "adamw_whole",
    )(*arrays, *gradients, *before)


def solution(mesh):
    def step(x, dy, *arrays):
        weights = arrays[:3]
        by0, hid0, h1, a1, a0 = forward(x[0], *weights)
        *gradients, pieces, _ = backward(a1, a0, dy[0], h1, by0, hid0, *weights)
        gathered = lax.all_gather(pieces, "dp")
        new = adamw_call(range(NG), arrays, gradients)
        return tuple(adamw_call(range(NG, NC), arrays, (gathered,), new))

    return jax.shard_map(
        step,
        mesh=mesh,
        in_specs=(P(("rep", "dp"), None, None),) * 2 + (P(None, None, None),) * 9,
        out_specs=(P("rep", None, None),) * 9,
        check_vma=False,
    )
```

```python
import jax
import jax.numpy as jnp
from jax import lax
from jax.experimental import pallas as pl
from jax.experimental.pallas import tpu as pltpu
from jax.sharding import PartitionSpec as P

BF, F32 = jnp.bfloat16, jnp.float32
T, D, FF = 2048, 1024, 3200
FC = 640
NF = FF // FC
NC = 2 * NF
TB = 512
NT = T // TB
NG = NF + 1
NK = NC - NG
BETWEEN = -1
RS = 3
VMEM_LIMIT = 67043328

AXES = (1, 8, 4, 2)
ORDER = (AXES, (1, 4, 2, 8), (1, 2, 8, 4))


def dot(a, b, ca, cb):
    return lax.dot_general(a, b, (((ca,), (cb,)), ((), ())), preferred_element_type=F32)


def inverse_rms(wide):
    return lax.rsqrt(jnp.mean(wide * wide, -1, keepdims=True) + 1e-6)


def gated(gate, up):
    s = 1.0 / (1.0 + jnp.exp(-gate))
    silu = gate * s
    return (silu * up).astype(BF), up * (s + silu * (1.0 - s)), silu


def split(a, b):
    return (a // b, a % b) if isinstance(a, int) else (lax.div(a, jnp.int32(b)), lax.rem(a, jnp.int32(b)))


def layer_and_start(c):
    before, chunk = split(c, NF)
    return 1 - before, chunk * FC


def any_spec(n):
    return [pl.BlockSpec(memory_space=pl.ANY)] * n


def forward_kernel(x, wg, wu, wd, by0, hid0, h1_ref, a1_ref, a0_ref, xb, wgu, wdv, hid, byb, xsem, wsem, dsem, osem, hsem):
    i = pl.program_id(0)
    rows = pl.ds(pl.multiple_of(i * TB, TB), TB)

    def columns(c):
        return pl.ds(pl.multiple_of(c * FC, 128), FC)

    def weights(c):
        return (
            pltpu.make_async_copy(wg.at[0, :, columns(c)], wgu.at[c, :, pl.ds(0, FC)], wsem.at[c, 0]),
            pltpu.make_async_copy(wu.at[0, :, columns(c)], wgu.at[c, :, pl.ds(FC, FC)], wsem.at[c, 1]),
        )

    down = pltpu.make_async_copy(wd.at[0], wdv, dsem)

    def tokens(n):
        return pltpu.make_async_copy(x.at[pl.ds(pl.multiple_of(n * TB, TB), TB), :], xb.at[lax.rem(n, 2)], xsem.at[lax.rem(n, 2)])

    @pl.when(i == 0)
    def _():
        tokens(i).start()
        for c in range(NF):
            for copy in weights(c):
                copy.start()
        down.start()

    def out_by(c):
        return pltpu.make_async_copy(byb.at[lax.rem(c, 2)], by0.at[c, rows, :], osem.at[lax.rem(c, 2)])

    def out_hid(c):
        return pltpu.make_async_copy(hid.at[:, columns(c)], hid0.at[c, rows, :], hsem.at[c])

    tokens(i).wait()

    @pl.when(i < NT - 1)
    def _():
        tokens(i + 1).start()

    wide = xb[lax.rem(i, 2)].astype(F32)
    a0_ref[...] = (wide * inverse_rms(wide)).astype(BF)

    def chunk(c, carry):
        @pl.when(i == 0)
        def _():
            for copy in weights(c):
                copy.wait()

        @pl.when(c >= 2)
        def _():
            out_by(c).wait()

        gu = dot(a0_ref[...], wgu[c], 1, 0)
        hid[:, columns(c)], byb[lax.rem(c, 2), :, :FC], byb[lax.rem(c, 2), :, FC:] = gated(gu[:, :FC], gu[:, FC:])
        out_by(c).start()
        out_hid(c).start()
        return carry

    lax.fori_loop(0, NF, chunk, 0)

    @pl.when(i == 0)
    def _():
        down.wait()

    h1_ref[...] = (xb[lax.rem(i, 2)].astype(F32) + dot(hid[...], wdv[...], 1, 0).astype(BF).astype(F32)).astype(BF)
    wide1 = h1_ref[...].astype(F32)
    a1_ref[...] = (wide1 * inverse_rms(wide1)).astype(BF)
    for c in range(NF):
        out_hid(c).wait()
    out_by(NF - 2).wait()
    out_by(NF - 1).wait()


def forward(x, wg, wu, wd):
    rows = pl.BlockSpec((TB, D), lambda i: (i, 0))
    dma = pltpu.SemaphoreType.DMA
    return pl.pallas_call(
        forward_kernel,
        grid=(NT,),
        out_shape=[
            jax.ShapeDtypeStruct((NF, T, 2 * FC), F32),
            jax.ShapeDtypeStruct((NF, T, FC), BF),
            jax.ShapeDtypeStruct((T, D), BF),
            jax.ShapeDtypeStruct((T, D), BF),
            jax.ShapeDtypeStruct((T, D), BF),
        ],
        in_specs=any_spec(4),
        out_specs=any_spec(2) + [rows] * 3,
        scratch_shapes=[
            pltpu.VMEM((2, TB, D), BF),
            pltpu.VMEM((NF, D, 2 * FC), BF),
            pltpu.VMEM((FF, D), BF),
            pltpu.VMEM((TB, FF), BF),
            pltpu.VMEM((2, TB, 2 * FC), F32),
            dma((2,)),
            dma((NF, 2)),
            dma,
            dma((2,)),
            dma((NF,)),
        ],
        compiler_params=pltpu.CompilerParams(dimension_semantics=("arbitrary",), vmem_limit_bytes=VMEM_LIMIT),
        cost_estimate=pl.CostEstimate(flops=6 * T * D * FF, bytes_accessed=110 << 20, transcendentals=T * FF),
        name="forward",
    )(x, wg, wu, wd)


def at(x, m):
    return x if isinstance(x, int) else pl.multiple_of(x, m)


class Sum:
    def __init__(self, g, out, pieces, recv_gate_up, recv_down, recv_down_ici, send, recv, gather_send, gather_recv, local, free):
        self.g, self.out, self.pieces = g, out, pieces
        self.recv_gate_up, self.recv_down, self.recv_down_ici = recv_gate_up, recv_down, recv_down_ici
        self.send, self.recv, self.local, self.free = send, recv, local, free
        self.gather_send, self.gather_recv = gather_send, gather_recv
        me = lax.axis_index("dp")
        bits = {b: split(split(me, b)[0], 2)[1] for b in AXES}
        self.core = bits[1]
        self.peers = {b: me + b * (1 - 2 * bits[b]) for b in AXES}
        self.origins = {}
        for p in range(3):
            row = column = 0
            self.origins[p, 0, False] = row, column
            for k, b in enumerate(ORDER[p]):
                for other in (True, False):
                    h = 1 - bits[b] if other else bits[b]
                    if p < 2:
                        here = row + h * (D // 2 >> k), column
                    elif k == 0:
                        here = row + h * (FC // 2), column
                    else:
                        here = row, column + h * (D >> k)
                    self.origins[p, k + 1, other] = here
                row, column = here

    def peer(self, b):
        return self.peers[b]

    def arrive(self):
        for b in AXES:
            pl.semaphore_signal(pltpu.get_barrier_semaphore(), inc=1, device_id={"dp": self.peer(b)})

    def meet(self):
        pl.semaphore_wait(pltpu.get_barrier_semaphore(), len(AXES))

    def origin(self, p, level, other=False):
        return self.origins[p, level, other]

    def shape(self, p, level):
        return (D >> level, FC) if p < 2 else (FC // 2, D >> (level - 1))

    def window(self, ref, origin, shape):
        return ref.at[pl.ds(at(origin[0], 64), shape[0]), pl.ds(at(origin[1], 128), shape[1])]

    def landing(self, p, k, slot):
        if p < 2:
            return self.recv_gate_up[p].at[slot, pl.ds(D - (D >> k), D // 2 >> k), :]
        if k == 0:
            return self.recv_down.at[slot]
        return self.recv_down_ici.at[slot, :, pl.ds(D - (D >> (k - 1)), D >> k)]

    def halve(self, p, c, k):
        slot = lax.rem(c, RS)
        return pltpu.make_async_remote_copy(
            src_ref=self.window(self.g[p].at[slot], self.origin(p, k + 1, other=True), self.shape(p, k + 1)),
            dst_ref=self.landing(p, k, slot),
            send_sem=self.send.at[slot, p, k],
            recv_sem=self.recv.at[slot, p, k],
            device_id={"dp": self.peer(ORDER[p][k])},
        )

    def place(self, p, c, origin, shape):
        layer, start = layer_and_start(c)
        if p < 2:
            return self.out[p].at[layer, pl.ds(at(origin[0], 64), shape[0]), pl.ds(pl.multiple_of(start, 128), FC)]
        return self.out[p].at[layer, pl.ds(pl.multiple_of(start + origin[0], 16), shape[0]), pl.ds(at(origin[1], 128), shape[1])]

    def gather(self, p, c, j, q=0):
        slot, level = lax.rem(c, RS), 4 - j
        (row, column), (rows, columns) = self.origin(p, level), self.shape(p, level)
        if j == 2:
            rows = rows // 4
            row = row + q * rows
        there = self.place(p, c, (row, column), (rows, columns))
        return pltpu.make_async_remote_copy(
            src_ref=self.window(self.g[p].at[slot], (row, column), (rows, columns)) if j == 0 else there,
            dst_ref=there,
            send_sem=self.gather_send.at[c, p, 3 + q if q else j],
            recv_sem=self.gather_recv.at[c, p, 3 + q if q else j],
            device_id={"dp": self.peer(ORDER[p][3 - j])},
        )

    def keep(self, p, c, piece):
        slot = lax.rem(c, RS)
        origin, shape = self.origin(p, 4), self.shape(p, 4)
        own, sem = self.window(self.g[p].at[slot], origin, shape), self.local.at[slot, p]
        if not piece:
            return [pltpu.make_async_copy(own, self.place(p, c, origin, shape), sem)]
        there = self.pieces.at[c - NG, p]
        if p < 2:
            return [pltpu.make_async_copy(own, there, sem)]
        return [pltpu.make_async_copy(own.at[pl.ds(64 * b, 64), :], there.at[:, pl.ds(128 * b, 128)], sem) for b in range(5)]

    def kept(self, p, c):
        slot = lax.rem(c, RS)
        there = self.pieces.at[0, 0]
        return pltpu.make_async_copy(self.g[0].at[slot, pl.ds(0, D // 16), :], there, self.local.at[slot, p])

    def add(self, p, c, k):
        slot = lax.rem(c, RS)
        level = min(k + 1, 4)
        (row, column), shape = self.origin(p, level, other=k < 4), self.shape(p, level)
        ref = self.g[p]
        if p < 2:

            def block(i, carry):
                here = (slot, pl.ds(pl.multiple_of(row + i * 64, 64), 64), slice(None))
                total = ref[here].astype(F32)
                for j in range(k):
                    there = D - (D >> j) + row - self.origin(p, j + 1)[0] + i * 64
                    total = total + self.recv_gate_up[p][slot, pl.ds(pl.multiple_of(there, 64), 64), :].astype(F32)
                ref[here] = total.astype(BF)
                return carry

            lax.fori_loop(0, shape[0] // 64, block, 0)
        else:

            def block(i, carry):
                here = (slot, pl.ds(pl.multiple_of(row, 64), shape[0]), pl.ds(pl.multiple_of(column + i * 128, 128), 128))
                total = ref[here].astype(F32)
                for j in range(k):
                    there = column - self.origin(p, j + 1)[1] + i * 128
                    if j == 0:
                        total = total + self.recv_down[slot, :, pl.ds(pl.multiple_of(there, 128), 128)].astype(F32)
                    else:
                        there = there + D - (D >> (j - 1))
                        total = total + self.recv_down_ici[slot, :, pl.ds(pl.multiple_of(there, 128), 128)].astype(F32)
                ref[here] = total.astype(BF)
                return carry

            lax.fori_loop(0, shape[1] // 128, block, 0)

    def step(self, k, q, parts, c, piece):
        group = parts[0] // 2
        if k < 2:

            @pl.when(c >= RS)
            def _():
                for axis in range(1) if k == 0 else range(1, 4):
                    pl.semaphore_wait(self.free.at[axis, group], 1)

        for p in parts:
            if 1 <= k <= 4:
                self.halve(p, c, k - 1).wait()
                self.add(p, c, k)
            if k < 4:
                self.halve(p, c, k).start()
            if k == 4:
                for copy in self.keep(p, c, piece):
                    copy.start()
            if k == 5:
                self.kept(p, c).wait()
            if k >= 5 and q == 0 and not piece:
                for quarter in range(4 if k == 7 else 1):
                    self.gather(p, c, k - 5, quarter).wait()
            if 4 <= k < 8 and not piece:
                self.gather(p, c, k - 4, q).start()
        if k == 4:

            @pl.when(c + RS < NC)
            def _():
                for axis, b in enumerate(AXES):
                    pl.semaphore_signal(self.free.at[axis, group], inc=1, device_id={"dp": self.peer(b)})


STEPS = [(i, step) for i in range(NF) for step in range(7)] + [(BETWEEN, step) for step in range(10)]
STEPS += [(i, step) for i in range(NF, NC + 8) for step in range(7)]

DIGITS = "0123456789abcdefghijklmnopqrstuvwxyzABCDEFGHIJKLMNOPQRSTUVWXYZ"
STAGES = [(k, q) for k in range(9) for q in range(4 if k == 6 else 1)]
TIMES = (
    ("57bdgjoxGOTV", "45begjlCHKPV"),
    ("57bdgjnnrxJQ", "47bdfjmrsDMU"),
    ("57bdgjnnrwJQ", "47bdfjmrsDMU"),
    ("56bdhkmmotxL", "57bdfimnszOW"),
    ("56bdfhqsswBQ", "46behjnopxIN"),
    ("56bdfjpqqryD", "45adijopqsxR"),
    ("57beko", "46beho"),
    ("58iqAD", "48fpBF"),
    ("56cpCE", "45bqzD"),
    ("59dkEO", "48clBW"),
)


def plan():
    entries = {}
    for c, both in enumerate(TIMES):
        for parts, times in zip(((0, 1), (2,)), both, strict=True):
            for (k, q), digit in zip(STAGES, times):
                entries.setdefault(STEPS[STEPS.index((c, 0)) + DIGITS.index(digit)], []).append((k, q, parts, c))
    return entries


def first(entry):
    k, q, parts, *_ = entry
    return (k > 4, -k if k <= 4 else k, q, parts)


PLAN = plan()
LAST, FIRST = range(NF), range(NF, NC)


def backward_kernel(
    a1, a0, dy, h1, by0, hid0, wg, wu, wd,
    out_gate, out_up, out_down, pieces, kept_dgu,
    a, by_h, by_a, wgu, wdv, hid, dgu, g_gate, g_up, g_down, recv_gate, recv_up, recv_down, recv_down_ici,
    rows_sem, load_sem, w_sem, by_sem, dgu_sem, send, recv, gather_send, gather_recv, local, free,
):
    total = Sum(
        (g_gate, g_up, g_down), (out_gate, out_up, out_down), pieces,
        (recv_gate, recv_up), recv_down, recv_down_ici, send, recv, gather_send, gather_recv, local, free,
    )

    def down_weights(c):
        (layer, start), slot = layer_and_start(c), lax.rem(c, 2)
        return [pltpu.make_async_copy(wd.at[layer, pl.ds(pl.multiple_of(start, 64), FC), :], wdv.at[slot], w_sem.at[slot, 2])]

    def input_weights(c):
        (layer, start), slot = layer_and_start(c), lax.rem(c, 2)
        columns = pl.ds(pl.multiple_of(start, 128), FC)
        return [
            pltpu.make_async_copy(w.at[layer, :, columns], wgu.at[slot, :, pl.ds(i * FC, FC)], w_sem.at[slot, i]) for i, w in enumerate((wg, wu))
        ]

    def rows_of(t):
        return pl.ds(pl.multiple_of(t * TB, TB), TB)

    def first_rows(t):
        return [
            pltpu.make_async_copy(dy.at[rows_of(t), :], by_h.at[rows_of(t), :], rows_sem.at[t, 0]),
            pltpu.make_async_copy(a1.at[rows_of(t), :], a.at[rows_of(t), :], rows_sem.at[t, 1]),
        ]

    def derivatives(c, t):
        return pltpu.make_async_copy(by0.at[c - NF, rows_of(t), :], by_a.at[rows_of(t), :], by_sem.at[t])

    def keep_dgu(c, t):
        return pltpu.make_async_copy(dgu.at[rows_of(t), :], kept_dgu.at[c, rows_of(t), :], dgu_sem.at[t])

    def fetch_dgu(c, t):
        return pltpu.make_async_copy(kept_dgu.at[c, rows_of(t), :], dgu.at[rows_of(t), :], dgu_sem.at[t])

    def hidden(c):
        return pltpu.make_async_copy(hid0.at[c - NF], hid, load_sem.at[2])

    load_h1 = pltpu.make_async_copy(h1, a, load_sem.at[0])
    load_a0 = pltpu.make_async_copy(a0, a, load_sem.at[1])

    total.arrive()
    for copy in down_weights(0) + input_weights(0) + first_rows(0):
        copy.start()
    by_a[:, :D] = jnp.zeros((T, D), F32)
    total.meet()

    def sends(step, c, span):
        found = {}
        for i in span:
            for k, q, parts, chunk in PLAN.get((i, step), ()):
                found.setdefault((k, q, parts, i - chunk, chunk >= NG), []).append(i)
        runs = []
        for entry, chunks in sorted(found.items(), key=lambda e: first(e[0])):
            for low in (i for i in chunks if i - 1 not in chunks):
                high = next(i for i in chunks if i >= low and i + 1 not in chunks)
                same = [run for run in runs if run[:2] == [low, high]]
                if same and all(run[0] > high or run[1] < low for run in runs[runs.index(same[-1]) + 1 :]):
                    same[-1][2].append(entry)
                else:
                    runs.append([low, high, [entry]])
        for low, high, entries in runs:

            @pl.when(jnp.logical_and(c >= low, c <= high))
            def _(entries=entries):
                for k, q, parts, back, piece in entries:
                    total.step(k, q, parts, c - back, piece)

    def sends_of_block(t, c, span):
        for n in range(NT):

            @pl.when(t == n)
            def _(n=n):
                sends(n, c, span)

    def weight_gradients(c, span):
        slot = lax.rem(c, RS)
        g_down[slot] = dot(hid[...], by_h[...], 0, 0).astype(BF)

        @pl.when(jnp.logical_and(c >= NF - 1, c < NC - 1))
        def _():
            hidden(c + 1).start()

        sends(4, c, span)

        def block(m, carry):
            half = jnp.where(m == 0, 1 - total.core, total.core)
            rows = pl.ds(pl.multiple_of(half * (D // 2), D // 2), D // 2)
            both = dot(a[:, rows], dgu[...], 0, 0).astype(BF)
            g_gate[slot, rows, :] = both[:, :FC]
            g_up[slot, rows, :] = both[:, FC:]

            @pl.when(m == 0)
            def _():
                sends(5, c, span)

            @pl.when(m == 1)
            def _():
                sends(6, c, span)

            return carry

        lax.fori_loop(0, 2, block, 0)

    def input_rows(t, slot):
        rows = rows_of(t)
        by_a[rows, :D] += dot(dgu[rows, :], wgu[slot], 1, 1)

    def last_layer(c, carry):
        slot = lax.rem(c, 2)
        for copy in down_weights(c) + input_weights(c):
            copy.wait()

        @pl.when(jnp.logical_and(c > 0, c < NF - 1))
        def _():
            for copy in down_weights(c + 1) + input_weights(c + 1):
                copy.start()

        @pl.when(c == NF - 1)
        def _():
            for copy in down_weights(c + 1):
                copy.start()

        def block(t, carry):
            @pl.when(c == 0)
            def _():
                for copy in first_rows(t):
                    copy.wait()

                @pl.when(t < NT - 1)
                def _():
                    for copy in first_rows(t + 1):
                        copy.start()

                @pl.when(t == NT - 1)
                def _():
                    for copy in down_weights(1) + input_weights(1):
                        copy.start()

            @pl.when(c > 0)
            def _():
                keep_dgu(c - 1, t).wait()

            rows = rows_of(t)
            gu = dot(a[rows, :], wgu[slot], 1, 0)
            by_hidden = dot(by_h[rows, :], wdv[slot], 1, 1).astype(BF).astype(F32)
            hid[rows, :], by_gate, by_up = gated(gu[:, :FC], gu[:, FC:])
            dgu[rows, :FC] = (by_hidden * by_gate).astype(BF)
            dgu[rows, FC:] = (by_hidden * by_up).astype(BF)

            @pl.when(c < NF - 1)
            def _():
                keep_dgu(c, t).start()

            sends_of_block(t, c, LAST)
            return carry

        lax.fori_loop(0, NT, block, 0)

        weight_gradients(c, LAST)

        return carry

    lax.fori_loop(0, NF, last_layer, 0)
    load_h1.start()

    def sends_between(step):
        for n in range(10):
            if (BETWEEN, n) in PLAN:

                @pl.when(step == n)
                def _(n=n):
                    for k, q, parts, chunk in sorted(PLAN[BETWEEN, n], key=first):
                        total.step(k, q, parts, chunk, chunk >= NG)

    def input_chunk(n, carry):
        c = NF - 1 - n
        slot = lax.rem(c, 2)

        @pl.when(n >= 2)
        def _():
            for copy in input_weights(c):
                copy.wait()

        @pl.when(jnp.logical_and(n >= 1, c > 0))
        def _():
            for copy in input_weights(c - 1):
                copy.start()

        def input_block(t, carry):
            @pl.when(n >= 1)
            def _():
                fetch_dgu(c, t).wait()

            input_rows(t, slot)

            @pl.when(c > 0)
            def _():
                fetch_dgu(c - 1, t).start()

            pair, odd = split(t, 2)

            @pl.when(odd == 1)
            def _():
                sends_between(2 * n + pair)

            return carry

        lax.fori_loop(0, jnp.where(c > 0, NT, 1), input_block, 0)
        return carry

    lax.fori_loop(0, NF, input_chunk, 0)
    load_h1.wait()

    def norm_rows(t):
        def some(n, carry):
            rows = pl.ds(pl.multiple_of(t * TB + n * 128, 128), 128)
            wide = a[rows, :].astype(F32)
            scale = inverse_rms(wide)
            by_normed = by_a[rows, :D].astype(BF).astype(F32)
            through = by_normed * scale - wide * (scale * scale * scale * jnp.mean(by_normed * wide, -1, keepdims=True))
            by_h[rows, :] = (by_h[rows, :].astype(F32) + through.astype(BF).astype(F32)).astype(BF)
            return carry

        lax.fori_loop(0, TB // 128, some, 0)

    def norm_block(t, carry):
        fetch_dgu(0, t).wait()
        norm_rows(t - 1)
        input_rows(t, 0)
        derivatives(NF, t - 1).start()

        pair, odd = split(t, 2)

        @pl.when(odd == 1)
        def _():
            sends_between(2 * (NF - 1) + pair)

        return carry

    lax.fori_loop(1, NT, norm_block, 0)
    norm_rows(NT - 1)
    derivatives(NF, NT - 1).start()
    load_a0.start()

    def first_layer(c, carry):
        slot = lax.rem(c, 2)
        for copy in down_weights(c):
            copy.wait()

        @pl.when(c < NC - 1)
        def _():
            for copy in down_weights(c + 1):
                copy.start()

        def block(t, carry):
            rows = rows_of(t)
            derivatives(c, t).wait()
            by_hidden = dot(by_h[rows, :], wdv[slot], 1, 1).astype(BF).astype(F32)
            dgu[rows, :FC] = (by_hidden * by_a[rows, :FC]).astype(BF)
            dgu[rows, FC:] = (by_hidden * by_a[rows, FC:]).astype(BF)

            @pl.when(c < NC - 1)
            def _():
                derivatives(c + 1, t).start()

            sends_of_block(t, c, FIRST)
            return carry

        lax.fori_loop(0, NT, block, 0)
        hidden(c).wait()

        @pl.when(c == NF)
        def _():
            load_a0.wait()

        weight_gradients(c, FIRST)
        return carry

    lax.fori_loop(NF, NC, first_layer, 0)
    for (i, _), entries in sorted(PLAN.items()):
        if i >= NC:
            for k, q, parts, chunk in sorted(entries, key=first):
                total.step(k, q, parts, chunk, chunk >= NG)


def backward(a1, a0, dy, h1, by0, hid0, wg, wu, wd):
    dma = pltpu.SemaphoreType.DMA
    return pl.pallas_call(
        backward_kernel,
        out_shape=[jax.ShapeDtypeStruct(shape, BF) for shape in ((2, D, FF), (2, D, FF), (2, FF, D), (NK, 3, D // 16, FC), (NF - 1, T, 2 * FC))],
        in_specs=any_spec(9),
        out_specs=any_spec(5),
        scratch_shapes=[
            pltpu.VMEM((T, D), BF),
            pltpu.VMEM((T, D), BF),
            pltpu.VMEM((T, 2 * FC), F32),
            pltpu.VMEM((2, D, 2 * FC), BF),
            pltpu.VMEM((2, FC, D), BF),
            pltpu.VMEM((T, FC), BF),
            pltpu.VMEM((T, 2 * FC), BF),
            pltpu.VMEM((RS, D, FC), BF),
            pltpu.VMEM((RS, D, FC), BF),
            pltpu.VMEM((RS, FC, D), BF),
            pltpu.VMEM((RS, D - D // 16, FC), BF),
            pltpu.VMEM((RS, D - D // 16, FC), BF),
            pltpu.VMEM((RS, FC // 2, D), BF),
            pltpu.VMEM((RS, FC // 2, D - D // 8), BF),
            dma((NT, 2)),
            dma((3,)),
            dma((2, 3)),
            dma((NT,)),
            dma((NT,)),
            dma((RS, 3, 4)),
            dma((RS, 3, 4)),
            dma((NG, 3, 7)),
            dma((NG, 3, 7)),
            dma((RS, 3)),
            pltpu.SemaphoreType.REGULAR((4, 2)),
        ],
        compiler_params=pltpu.CompilerParams(collective_id=0, has_side_effects=True, vmem_limit_bytes=VMEM_LIMIT),
        cost_estimate=pl.CostEstimate(flops=24 * T * D * FF, bytes_accessed=200 << 20, transcendentals=2 * T * FF),
        name="backward",
    )(a1, a0, dy, h1, by0, hid0, wg, wu, wd)


SLOTS = 4
HALVES = ((D // 2, FC), (D // 2, FC), (FC // 2, D))


def adamw(w, m, v, g):
    m = 0.9 * m + 0.1 * g
    v = 0.95 * v + 0.05 * g * g
    step = m * lax.rsqrt(v + 1e-8) + 0.1 * w
    return (w - 0.02 * step).astype(BF), m, v


def owner(p, half, q):
    bits = ORDER[p]
    return half * bits[0] + q // 4 * bits[1] + q // 2 % 2 * bits[2] + q % 2 * bits[3]


def adamw_kernel(chunks, in_pieces, n_before, *refs):
    w, m, v = refs[0:3], refs[3:6], refs[6:9]
    n_g = 1 if in_pieces else 3
    g, outs = refs[9 : 9 + n_g], refs[9 + n_g + n_before : 18 + n_g + n_before]
    *bufs, load_sem, store_sem = refs[18 + n_g + n_before :]
    units, units_before = 2 * len(chunks), 2 * chunks[0]

    def window(ref, p, c, half):
        rows, columns = HALVES[p]
        layer, start = layer_and_start(c)
        if p < 2:
            return ref.at[layer, pl.ds(pl.multiple_of(half * rows, rows), rows), pl.ds(pl.multiple_of(start, 128), FC)]
        return ref.at[layer, pl.ds(pl.multiple_of(start + half * rows, 64), rows), :]

    def gradient(p, c, half, to, sem):
        if not in_pieces:
            return [pltpu.make_async_copy(window(g[p], p, c, half), to, sem)]
        copies = []
        for e in range(8):
            piece = g[0].at[owner(p, half, e), c - NG, p]
            if p < 2:
                copies.append(pltpu.make_async_copy(piece, to.at[pl.ds(64 * e, 64), :], sem))
            else:
                for b in range(5):
                    there = to.at[pl.ds(64 * b, 64), pl.ds(128 * e, 128)]
                    copies.append(pltpu.make_async_copy(piece.at[:, pl.ds(128 * b, 128)], there, sem))
        return copies

    def loads(n, act):
        (c, half), slot = split(n + units_before, 2), lax.rem(n, SLOTS)
        for p in range(3):
            for b, ref in enumerate((w[p], m[p], v[p])):
                copy = pltpu.make_async_copy(window(ref, p, c, half), bufs[4 * p + b].at[slot], load_sem.at[slot, p, b])
                copy.start() if act == "start" else copy.wait()
            to, sem = bufs[4 * p + 3].at[slot], load_sem.at[slot, p, 3]
            if act == "start":
                for copy in gradient(p, c, half, to, sem):
                    copy.start()
            else:
                pltpu.make_async_copy(window(w[p], p, c, half), to, sem).wait()

    def stores(n, act):
        (c, half), slot = split(n + units_before, 2), lax.rem(n, SLOTS)
        for p in range(3):
            for b in range(3):
                copy = pltpu.make_async_copy(bufs[4 * p + b].at[slot], window(outs[3 * b + p], p, c, half), store_sem.at[slot, p, b])
                copy.start() if act == "start" else copy.wait()

    loads(0, "start")
    loads(1, "start")

    def unit(n, carry):
        slot = lax.rem(n, SLOTS)

        @pl.when(n >= 2)
        def _():
            stores(n - 2, "wait")

        loads(n, "wait")

        @pl.when(n + 2 < units)
        def _():
            loads(n + 2, "start")

        for p in range(3):
            block = 64 if p < 2 else 32

            def rows_block(r, carry, buf=bufs[4 * p : 4 * p + 4], block=block):
                here = (slot, pl.ds(pl.multiple_of(r * block, block), block), slice(None))
                buf[0][here], buf[1][here], buf[2][here] = adamw(
                    buf[0][here].astype(F32), buf[1][here], buf[2][here], buf[3][here].astype(F32)
                )
                return carry

            lax.fori_loop(0, HALVES[p][0] // block, rows_block, 0)
        stores(n, "start")
        return carry

    lax.fori_loop(0, units, unit, 0)
    stores(units - 2, "wait")
    stores(units - 1, "wait")


def adamw_call(chunks, arrays, gradients, before=()):
    in_pieces, n_before = len(gradients) == 1, len(before)

    def kernel(*refs):
        adamw_kernel(chunks, in_pieces, n_before, *refs)

    elements, n_in = 3 * D * FC * len(chunks), 9 + len(gradients)
    return pl.pallas_call(
        kernel,
        out_shape=[jax.ShapeDtypeStruct(a.shape, a.dtype) for a in arrays],
        in_specs=any_spec(n_in + n_before),
        out_specs=any_spec(9),
        input_output_aliases={n_in + i: i for i in range(n_before)},
        scratch_shapes=[pltpu.VMEM((SLOTS, *shape), t) for shape in HALVES for t in (BF, F32, F32, BF)]
        + [pltpu.SemaphoreType.DMA((SLOTS, 3, 4)), pltpu.SemaphoreType.DMA((SLOTS, 3, 3))],
        compiler_params=pltpu.CompilerParams(vmem_limit_bytes=VMEM_LIMIT),
        cost_estimate=pl.CostEstimate(flops=15 * elements, bytes_accessed=22 * elements, transcendentals=elements),
        name="adamw_pieces" if in_pieces else "adamw_whole",
    )(*arrays, *gradients, *before)


def solution(mesh):
    def step(x, dy, *arrays):
        weights = arrays[:3]
        by0, hid0, h1, a1, a0 = forward(x[0], *weights)
        *gradients, pieces, _ = backward(a1, a0, dy[0], h1, by0, hid0, *weights)
        gathered = lax.all_gather(pieces, "dp")
        new = adamw_call(range(NG), arrays, gradients)
        return tuple(adamw_call(range(NG, NC), arrays, (gathered,), new))

    return jax.shard_map(
        step,
        mesh=mesh,
        in_specs=(P(("rep", "dp"), None, None),) * 2 + (P(None, None, None),) * 9,
        out_specs=(P("rep", None, None),) * 9,
        check_vma=False,
    )
```

```python
import jax
import jax.numpy as jnp
from jax import lax
from jax.experimental import pallas as pl
from jax.experimental.pallas import tpu as pltpu
from jax.sharding import PartitionSpec as P

BF, F32 = jnp.bfloat16, jnp.float32
T, D, FF = 2048, 1024, 3200
FC = 640
NF = FF // FC
NC = 2 * NF
TB = 512
NT = T // TB
NG = NF + 1
NK = NC - NG
BETWEEN = -1
RS = 3
VMEM_LIMIT = 67043328

AXES = (1, 8, 4, 2)
ORDER = (AXES, (1, 4, 2, 8), (1, 2, 8, 4))


def dot(a, b, ca, cb):
    return lax.dot_general(a, b, (((ca,), (cb,)), ((), ())), preferred_element_type=F32)


def inverse_rms(wide):
    return lax.rsqrt(jnp.mean(wide * wide, -1, keepdims=True) + 1e-6)


def gated(gate, up):
    s = 1.0 / (1.0 + jnp.exp(-gate))
    silu = gate * s
    return (silu * up).astype(BF), up * (s + silu * (1.0 - s)), silu


def split(a, b):
    return (a // b, a % b) if isinstance(a, int) else (lax.div(a, jnp.int32(b)), lax.rem(a, jnp.int32(b)))


def layer_and_start(c):
    before, chunk = split(c, NF)
    return 1 - before, chunk * FC


def any_spec(n):
    return [pl.BlockSpec(memory_space=pl.ANY)] * n


def forward_kernel(x, wg, wu, wd, by0, hid0, h1_ref, a1_ref, a0_ref, xb, wgu, wdv, hid, byb, xsem, wsem, dsem, osem, hsem):
    i = pl.program_id(0)
    rows = pl.ds(pl.multiple_of(i * TB, TB), TB)

    def columns(c):
        return pl.ds(pl.multiple_of(c * FC, 128), FC)

    def weights(c):
        return (
            pltpu.make_async_copy(wg.at[0, :, columns(c)], wgu.at[c, :, pl.ds(0, FC)], wsem.at[c, 0]),
            pltpu.make_async_copy(wu.at[0, :, columns(c)], wgu.at[c, :, pl.ds(FC, FC)], wsem.at[c, 1]),
        )

    down = pltpu.make_async_copy(wd.at[0], wdv, dsem)

    def tokens(n):
        return pltpu.make_async_copy(x.at[pl.ds(pl.multiple_of(n * TB, TB), TB), :], xb.at[lax.rem(n, 2)], xsem.at[lax.rem(n, 2)])

    @pl.when(i == 0)
    def _():
        tokens(i).start()
        for c in range(NF):
            for copy in weights(c):
                copy.start()
        down.start()

    def out_by(c):
        return pltpu.make_async_copy(byb.at[lax.rem(c, 2)], by0.at[c, rows, :], osem.at[lax.rem(c, 2)])

    def out_hid(c):
        return pltpu.make_async_copy(hid.at[:, columns(c)], hid0.at[c, rows, :], hsem.at[c])

    tokens(i).wait()

    @pl.when(i < NT - 1)
    def _():
        tokens(i + 1).start()

    wide = xb[lax.rem(i, 2)].astype(F32)
    a0_ref[...] = (wide * inverse_rms(wide)).astype(BF)

    def chunk(c, carry):
        @pl.when(i == 0)
        def _():
            for copy in weights(c):
                copy.wait()

        @pl.when(c >= 2)
        def _():
            out_by(c).wait()

        gu = dot(a0_ref[...], wgu[c], 1, 0)
        hid[:, columns(c)], byb[lax.rem(c, 2), :, :FC], byb[lax.rem(c, 2), :, FC:] = gated(gu[:, :FC], gu[:, FC:])
        out_by(c).start()
        out_hid(c).start()
        return carry

    lax.fori_loop(0, NF, chunk, 0)

    @pl.when(i == 0)
    def _():
        down.wait()

    h1_ref[...] = (xb[lax.rem(i, 2)].astype(F32) + dot(hid[...], wdv[...], 1, 0).astype(BF).astype(F32)).astype(BF)
    wide1 = h1_ref[...].astype(F32)
    a1_ref[...] = (wide1 * inverse_rms(wide1)).astype(BF)
    for c in range(NF):
        out_hid(c).wait()
    out_by(NF - 2).wait()
    out_by(NF - 1).wait()


def forward(x, wg, wu, wd):
    rows = pl.BlockSpec((TB, D), lambda i: (i, 0))
    dma = pltpu.SemaphoreType.DMA
    return pl.pallas_call(
        forward_kernel,
        grid=(NT,),
        out_shape=[
            jax.ShapeDtypeStruct((NF, T, 2 * FC), F32),
            jax.ShapeDtypeStruct((NF, T, FC), BF),
            jax.ShapeDtypeStruct((T, D), BF),
            jax.ShapeDtypeStruct((T, D), BF),
            jax.ShapeDtypeStruct((T, D), BF),
        ],
        in_specs=any_spec(4),
        out_specs=any_spec(2) + [rows] * 3,
        scratch_shapes=[
            pltpu.VMEM((2, TB, D), BF),
            pltpu.VMEM((NF, D, 2 * FC), BF),
            pltpu.VMEM((FF, D), BF),
            pltpu.VMEM((TB, FF), BF),
            pltpu.VMEM((2, TB, 2 * FC), F32),
            dma((2,)),
            dma((NF, 2)),
            dma,
            dma((2,)),
            dma((NF,)),
        ],
        compiler_params=pltpu.CompilerParams(dimension_semantics=("arbitrary",), vmem_limit_bytes=VMEM_LIMIT),
        cost_estimate=pl.CostEstimate(flops=6 * T * D * FF, bytes_accessed=110 << 20, transcendentals=T * FF),
        name="forward",
    )(x, wg, wu, wd)


def at(x, m):
    return x if isinstance(x, int) else pl.multiple_of(x, m)


class Sum:
    def __init__(self, g, out, pieces, recv_gate_up, recv_down, recv_down_ici, send, recv, gather_send, gather_recv, local, free):
        self.g, self.out, self.pieces = g, out, pieces
        self.recv_gate_up, self.recv_down, self.recv_down_ici = recv_gate_up, recv_down, recv_down_ici
        self.send, self.recv, self.local, self.free = send, recv, local, free
        self.gather_send, self.gather_recv = gather_send, gather_recv
        me = lax.axis_index("dp")
        bits = {b: split(split(me, b)[0], 2)[1] for b in AXES}
        self.core = bits[1]
        self.peers = {b: me + b * (1 - 2 * bits[b]) for b in AXES}
        self.origins = {}
        for p in range(3):
            row = column = 0
            self.origins[p, 0, False] = row, column
            for k, b in enumerate(ORDER[p]):
                for other in (True, False):
                    h = 1 - bits[b] if other else bits[b]
                    if p < 2:
                        here = row + h * (D // 2 >> k), column
                    elif k == 0:
                        here = row + h * (FC // 2), column
                    else:
                        here = row, column + h * (D >> k)
                    self.origins[p, k + 1, other] = here
                row, column = here

    def peer(self, b):
        return self.peers[b]

    def arrive(self):
        for b in AXES:
            pl.semaphore_signal(pltpu.get_barrier_semaphore(), inc=1, device_id={"dp": self.peer(b)})

    def meet(self):
        pl.semaphore_wait(pltpu.get_barrier_semaphore(), len(AXES))

    def origin(self, p, level, other=False):
        return self.origins[p, level, other]

    def shape(self, p, level):
        return (D >> level, FC) if p < 2 else (FC // 2, D >> (level - 1))

    def window(self, ref, origin, shape):
        return ref.at[pl.ds(at(origin[0], 64), shape[0]), pl.ds(at(origin[1], 128), shape[1])]

    def landing(self, p, k, slot):
        if p < 2:
            return self.recv_gate_up[p].at[slot, pl.ds(D - (D >> k), D // 2 >> k), :]
        if k == 0:
            return self.recv_down.at[slot]
        return self.recv_down_ici.at[slot, :, pl.ds(D - (D >> (k - 1)), D >> k)]

    def halve(self, p, c, k):
        slot = lax.rem(c, RS)
        return pltpu.make_async_remote_copy(
            src_ref=self.window(self.g[p].at[slot], self.origin(p, k + 1, other=True), self.shape(p, k + 1)),
            dst_ref=self.landing(p, k, slot),
            send_sem=self.send.at[slot, p, k],
            recv_sem=self.recv.at[slot, p, k],
            device_id={"dp": self.peer(ORDER[p][k])},
        )

    def place(self, p, c, origin, shape):
        layer, start = layer_and_start(c)
        if p < 2:
            return self.out[p].at[layer, pl.ds(at(origin[0], 64), shape[0]), pl.ds(pl.multiple_of(start, 128), FC)]
        return self.out[p].at[layer, pl.ds(pl.multiple_of(start + origin[0], 16), shape[0]), pl.ds(at(origin[1], 128), shape[1])]

    def gather(self, p, c, j, q=0):
        slot, level = lax.rem(c, RS), 4 - j
        (row, column), (rows, columns) = self.origin(p, level), self.shape(p, level)
        if j == 2:
            rows = rows // 4
            row = row + q * rows
        there = self.place(p, c, (row, column), (rows, columns))
        return pltpu.make_async_remote_copy(
            src_ref=self.window(self.g[p].at[slot], (row, column), (rows, columns)) if j == 0 else there,
            dst_ref=there,
            send_sem=self.gather_send.at[c, p, 3 + q if q else j],
            recv_sem=self.gather_recv.at[c, p, 3 + q if q else j],
            device_id={"dp": self.peer(ORDER[p][3 - j])},
        )

    def keep(self, p, c, piece):
        slot = lax.rem(c, RS)
        origin, shape = self.origin(p, 4), self.shape(p, 4)
        own, sem = self.window(self.g[p].at[slot], origin, shape), self.local.at[slot, p]
        if not piece:
            return [pltpu.make_async_copy(own, self.place(p, c, origin, shape), sem)]
        there = self.pieces.at[c - NG, p]
        if p < 2:
            return [pltpu.make_async_copy(own, there, sem)]
        return [pltpu.make_async_copy(own.at[pl.ds(64 * b, 64), :], there.at[:, pl.ds(128 * b, 128)], sem) for b in range(5)]

    def kept(self, p, c):
        slot = lax.rem(c, RS)
        there = self.pieces.at[0, 0]
        return pltpu.make_async_copy(self.g[0].at[slot, pl.ds(0, D // 16), :], there, self.local.at[slot, p])

    def add(self, p, c, k):
        slot = lax.rem(c, RS)
        level = min(k + 1, 4)
        (row, column), shape = self.origin(p, level, other=k < 4), self.shape(p, level)
        ref = self.g[p]
        if p < 2:

            def block(i, carry):
                here = (slot, pl.ds(pl.multiple_of(row + i * 64, 64), 64), slice(None))
                total = ref[here].astype(F32)
                for j in range(k):
                    there = D - (D >> j) + row - self.origin(p, j + 1)[0] + i * 64
                    total = total + self.recv_gate_up[p][slot, pl.ds(pl.multiple_of(there, 64), 64), :].astype(F32)
                ref[here] = total.astype(BF)
                return carry

            lax.fori_loop(0, shape[0] // 64, block, 0)
        else:

            def block(i, carry):
                here = (slot, pl.ds(pl.multiple_of(row, 64), shape[0]), pl.ds(pl.multiple_of(column + i * 128, 128), 128))
                total = ref[here].astype(F32)
                for j in range(k):
                    there = column - self.origin(p, j + 1)[1] + i * 128
                    if j == 0:
                        total = total + self.recv_down[slot, :, pl.ds(pl.multiple_of(there, 128), 128)].astype(F32)
                    else:
                        there = there + D - (D >> (j - 1))
                        total = total + self.recv_down_ici[slot, :, pl.ds(pl.multiple_of(there, 128), 128)].astype(F32)
                ref[here] = total.astype(BF)
                return carry

            lax.fori_loop(0, shape[1] // 128, block, 0)

    def step(self, k, q, parts, c, piece):
        group = parts[0] // 2
        if k < 2:

            @pl.when(c >= RS)
            def _():
                for axis in range(1) if k == 0 else range(1, 4):
                    pl.semaphore_wait(self.free.at[axis, group], 1)

        for p in parts:
            if 1 <= k <= 4:
                self.halve(p, c, k - 1).wait()
                self.add(p, c, k)
            if k < 4:
                self.halve(p, c, k).start()
            if k == 4:
                for copy in self.keep(p, c, piece):
                    copy.start()
            if k == 5:
                self.kept(p, c).wait()
            if k >= 5 and q == 0 and not piece:
                for quarter in range(4 if k == 7 else 1):
                    self.gather(p, c, k - 5, quarter).wait()
            if 4 <= k < 8 and not piece:
                self.gather(p, c, k - 4, q).start()
        if k == 4:

            @pl.when(c + RS < NC)
            def _():
                for axis, b in enumerate(AXES):
                    pl.semaphore_signal(self.free.at[axis, group], inc=1, device_id={"dp": self.peer(b)})


STEPS = [(i, step) for i in range(NF) for step in range(7)] + [(BETWEEN, step) for step in range(10)]
STEPS += [(i, step) for i in range(NF, NC + 8) for step in range(7)]

DIGITS = "0123456789abcdefghijklmnopqrstuvwxyzABCDEFGHIJKLMNOPQRSTUVWXYZ"
STAGES = [(k, q) for k in range(9) for q in range(4 if k == 6 else 1)]
TIMES = (
    ("57bdfjovBMRX", "47cehjorIJRV"),
    ("57bdgjpqtwJV", "57bdhjpqstJS"),
    ("57bdgjpqtvJV", "57bdhjpqstJS"),
    ("57bfilnootOV", "47beglorszBN"),
    ("57bdfgmqrxRT", "45adgjoopxCF"),
    ("57cgijnnnsxO", "45adgjppqqAW"),
    ("56belo", "45bdkl"),
    ("57imzB", "57ipxH"),
    ("56cmrA", "57cltz"),
    ("57dgPR", "46chHP"),
)


def plan():
    entries = {}
    for c, both in enumerate(TIMES):
        for parts, times in zip(((0, 1), (2,)), both, strict=True):
            for (k, q), digit in zip(STAGES, times):
                entries.setdefault(STEPS[STEPS.index((c, 0)) + DIGITS.index(digit)], []).append((k, q, parts, c))
    return entries


def first(entry):
    k, q, parts, *_ = entry
    return (k > 4, -k if k <= 4 else k, q, parts)


PLAN = plan()
LAST, FIRST = range(NF), range(NF, NC)


def backward_kernel(
    a1, a0, dy, h1, by0, hid0, wg, wu, wd,
    out_gate, out_up, out_down, pieces, kept_dgu,
    a, by_h, by_a, wgu, wdv, hid, dgu, g_gate, g_up, g_down, recv_gate, recv_up, recv_down, recv_down_ici,
    rows_sem, load_sem, w_sem, by_sem, dgu_sem, send, recv, gather_send, gather_recv, local, free,
):
    total = Sum(
        (g_gate, g_up, g_down), (out_gate, out_up, out_down), pieces,
        (recv_gate, recv_up), recv_down, recv_down_ici, send, recv, gather_send, gather_recv, local, free,
    )

    def down_weights(c):
        (layer, start), slot = layer_and_start(c), lax.rem(c, 2)
        return [pltpu.make_async_copy(wd.at[layer, pl.ds(pl.multiple_of(start, 64), FC), :], wdv.at[slot], w_sem.at[slot, 2])]

    def input_weights(c):
        (layer, start), slot = layer_and_start(c), lax.rem(c, 2)
        columns = pl.ds(pl.multiple_of(start, 128), FC)
        return [
            pltpu.make_async_copy(w.at[layer, :, columns], wgu.at[slot, :, pl.ds(i * FC, FC)], w_sem.at[slot, i]) for i, w in enumerate((wg, wu))
        ]

    def rows_of(t):
        return pl.ds(pl.multiple_of(t * TB, TB), TB)

    def first_rows(t):
        return [
            pltpu.make_async_copy(dy.at[rows_of(t), :], by_h.at[rows_of(t), :], rows_sem.at[t, 0]),
            pltpu.make_async_copy(a1.at[rows_of(t), :], a.at[rows_of(t), :], rows_sem.at[t, 1]),
        ]

    def derivatives(c, t):
        return pltpu.make_async_copy(by0.at[c - NF, rows_of(t), :], by_a.at[rows_of(t), :], by_sem.at[t])

    def keep_dgu(c, t):
        return pltpu.make_async_copy(dgu.at[rows_of(t), :], kept_dgu.at[c, rows_of(t), :], dgu_sem.at[t])

    def fetch_dgu(c, t):
        return pltpu.make_async_copy(kept_dgu.at[c, rows_of(t), :], dgu.at[rows_of(t), :], dgu_sem.at[t])

    def hidden(c):
        return pltpu.make_async_copy(hid0.at[c - NF], hid, load_sem.at[2])

    load_h1 = pltpu.make_async_copy(h1, a, load_sem.at[0])
    load_a0 = pltpu.make_async_copy(a0, a, load_sem.at[1])

    total.arrive()
    for copy in down_weights(0) + input_weights(0) + first_rows(0):
        copy.start()
    by_a[:, :D] = jnp.zeros((T, D), F32)
    total.meet()

    def sends(step, c, span):
        found = {}
        for i in span:
            for k, q, parts, chunk in PLAN.get((i, step), ()):
                found.setdefault((k, q, parts, i - chunk, chunk >= NG), []).append(i)
        runs = []
        for entry, chunks in sorted(found.items(), key=lambda e: first(e[0])):
            for low in (i for i in chunks if i - 1 not in chunks):
                high = next(i for i in chunks if i >= low and i + 1 not in chunks)
                same = [run for run in runs if run[:2] == [low, high]]
                if same and all(run[0] > high or run[1] < low for run in runs[runs.index(same[-1]) + 1 :]):
                    same[-1][2].append(entry)
                else:
                    runs.append([low, high, [entry]])
        for low, high, entries in runs:

            @pl.when(jnp.logical_and(c >= low, c <= high))
            def _(entries=entries):
                for k, q, parts, back, piece in entries:
                    total.step(k, q, parts, c - back, piece)

    def sends_of_block(t, c, span):
        for n in range(NT):

            @pl.when(t == n)
            def _(n=n):
                sends(n, c, span)

    def weight_gradients(c, span):
        slot = lax.rem(c, RS)
        g_down[slot] = dot(hid[...], by_h[...], 0, 0).astype(BF)

        @pl.when(jnp.logical_and(c >= NF - 1, c < NC - 1))
        def _():
            hidden(c + 1).start()

        sends(4, c, span)

        def block(m, carry):
            half = jnp.where(m == 0, 1 - total.core, total.core)
            rows = pl.ds(pl.multiple_of(half * (D // 2), D // 2), D // 2)
            both = dot(a[:, rows], dgu[...], 0, 0).astype(BF)
            g_gate[slot, rows, :] = both[:, :FC]
            g_up[slot, rows, :] = both[:, FC:]

            @pl.when(m == 0)
            def _():
                sends(5, c, span)

            @pl.when(m == 1)
            def _():
                sends(6, c, span)

            return carry

        lax.fori_loop(0, 2, block, 0)

    def input_rows(t, slot):
        rows = rows_of(t)
        by_a[rows, :D] += dot(dgu[rows, :], wgu[slot], 1, 1)

    def last_layer(c, carry):
        slot = lax.rem(c, 2)
        for copy in down_weights(c) + input_weights(c):
            copy.wait()

        @pl.when(jnp.logical_and(c > 0, c < NF - 1))
        def _():
            for copy in down_weights(c + 1) + input_weights(c + 1):
                copy.start()

        @pl.when(c == NF - 1)
        def _():
            for copy in down_weights(c + 1):
                copy.start()

        def block(t, carry):
            @pl.when(c == 0)
            def _():
                for copy in first_rows(t):
                    copy.wait()

                @pl.when(t < NT - 1)
                def _():
                    for copy in first_rows(t + 1):
                        copy.start()

                @pl.when(t == NT - 1)
                def _():
                    for copy in down_weights(1) + input_weights(1):
                        copy.start()

            @pl.when(c > 0)
            def _():
                keep_dgu(c - 1, t).wait()

            rows = rows_of(t)
            gu = dot(a[rows, :], wgu[slot], 1, 0)
            by_hidden = dot(by_h[rows, :], wdv[slot], 1, 1).astype(BF).astype(F32)
            hid[rows, :], by_gate, by_up = gated(gu[:, :FC], gu[:, FC:])
            dgu[rows, :FC] = (by_hidden * by_gate).astype(BF)
            dgu[rows, FC:] = (by_hidden * by_up).astype(BF)

            @pl.when(c < NF - 1)
            def _():
                keep_dgu(c, t).start()

            sends_of_block(t, c, LAST)
            return carry

        lax.fori_loop(0, NT, block, 0)

        weight_gradients(c, LAST)

        return carry

    lax.fori_loop(0, NF, last_layer, 0)
    load_h1.start()

    def sends_between(step):
        for n in range(10):
            if (BETWEEN, n) in PLAN:

                @pl.when(step == n)
                def _(n=n):
                    for k, q, parts, chunk in sorted(PLAN[BETWEEN, n], key=first):
                        total.step(k, q, parts, chunk, chunk >= NG)

    def input_chunk(n, carry):
        c = NF - 1 - n
        slot = lax.rem(c, 2)

        @pl.when(n >= 2)
        def _():
            for copy in input_weights(c):
                copy.wait()

        @pl.when(jnp.logical_and(n >= 1, c > 0))
        def _():
            for copy in input_weights(c - 1):
                copy.start()

        def input_block(t, carry):
            @pl.when(n >= 1)
            def _():
                fetch_dgu(c, t).wait()

            input_rows(t, slot)

            @pl.when(c > 0)
            def _():
                fetch_dgu(c - 1, t).start()

            pair, odd = split(t, 2)

            @pl.when(odd == 1)
            def _():
                sends_between(2 * n + pair)

            return carry

        lax.fori_loop(0, jnp.where(c > 0, NT, 1), input_block, 0)
        return carry

    lax.fori_loop(0, NF, input_chunk, 0)
    load_h1.wait()

    def norm_rows(t):
        def some(n, carry):
            rows = pl.ds(pl.multiple_of(t * TB + n * 256, 256), 256)
            wide = a[rows, :].astype(F32)
            scale = inverse_rms(wide)
            by_normed = by_a[rows, :D].astype(BF).astype(F32)
            through = by_normed * scale - wide * (scale * scale * scale * jnp.mean(by_normed * wide, -1, keepdims=True))
            by_h[rows, :] = (by_h[rows, :].astype(F32) + through.astype(BF).astype(F32)).astype(BF)
            return carry

        lax.fori_loop(0, TB // 256, some, 0)

    def norm_block(t, carry):
        fetch_dgu(0, t).wait()
        norm_rows(t - 1)
        input_rows(t, 0)
        derivatives(NF, t - 1).start()

        pair, odd = split(t, 2)

        @pl.when(odd == 1)
        def _():
            sends_between(2 * (NF - 1) + pair)

        return carry

    lax.fori_loop(1, NT, norm_block, 0)
    norm_rows(NT - 1)
    derivatives(NF, NT - 1).start()
    load_a0.start()

    def first_layer(c, carry):
        slot = lax.rem(c, 2)
        for copy in down_weights(c):
            copy.wait()

        @pl.when(c < NC - 1)
        def _():
            for copy in down_weights(c + 1):
                copy.start()

        def block(t, carry):
            rows = rows_of(t)
            derivatives(c, t).wait()
            by_hidden = dot(by_h[rows, :], wdv[slot], 1, 1).astype(BF).astype(F32)
            dgu[rows, :FC] = (by_hidden * by_a[rows, :FC]).astype(BF)
            dgu[rows, FC:] = (by_hidden * by_a[rows, FC:]).astype(BF)

            @pl.when(c < NC - 1)
            def _():
                derivatives(c + 1, t).start()

            sends_of_block(t, c, FIRST)
            return carry

        lax.fori_loop(0, NT, block, 0)
        hidden(c).wait()

        @pl.when(c == NF)
        def _():
            load_a0.wait()

        weight_gradients(c, FIRST)
        return carry

    lax.fori_loop(NF, NC, first_layer, 0)
    for (i, _), entries in sorted(PLAN.items()):
        if i >= NC:
            for k, q, parts, chunk in sorted(entries, key=first):
                total.step(k, q, parts, chunk, chunk >= NG)


def backward(a1, a0, dy, h1, by0, hid0, wg, wu, wd):
    dma = pltpu.SemaphoreType.DMA
    return pl.pallas_call(
        backward_kernel,
        out_shape=[jax.ShapeDtypeStruct(shape, BF) for shape in ((2, D, FF), (2, D, FF), (2, FF, D), (NK, 3, D // 16, FC), (NF - 1, T, 2 * FC))],
        in_specs=any_spec(9),
        out_specs=any_spec(5),
        scratch_shapes=[
            pltpu.VMEM((T, D), BF),
            pltpu.VMEM((T, D), BF),
            pltpu.VMEM((T, 2 * FC), F32),
            pltpu.VMEM((2, D, 2 * FC), BF),
            pltpu.VMEM((2, FC, D), BF),
            pltpu.VMEM((T, FC), BF),
            pltpu.VMEM((T, 2 * FC), BF),
            pltpu.VMEM((RS, D, FC), BF),
            pltpu.VMEM((RS, D, FC), BF),
            pltpu.VMEM((RS, FC, D), BF),
            pltpu.VMEM((RS, D - D // 16, FC), BF),
            pltpu.VMEM((RS, D - D // 16, FC), BF),
            pltpu.VMEM((RS, FC // 2, D), BF),
            pltpu.VMEM((RS, FC // 2, D - D // 8), BF),
            dma((NT, 2)),
            dma((3,)),
            dma((2, 3)),
            dma((NT,)),
            dma((NT,)),
            dma((RS, 3, 4)),
            dma((RS, 3, 4)),
            dma((NG, 3, 7)),
            dma((NG, 3, 7)),
            dma((RS, 3)),
            pltpu.SemaphoreType.REGULAR((4, 2)),
        ],
        compiler_params=pltpu.CompilerParams(collective_id=0, has_side_effects=True, vmem_limit_bytes=VMEM_LIMIT),
        cost_estimate=pl.CostEstimate(flops=24 * T * D * FF, bytes_accessed=200 << 20, transcendentals=2 * T * FF),
        name="backward",
    )(a1, a0, dy, h1, by0, hid0, wg, wu, wd)


SLOTS = 4
HALVES = ((D // 2, FC), (D // 2, FC), (FC // 2, D))


def adamw(w, m, v, g):
    m = 0.9 * m + 0.1 * g
    v = 0.95 * v + 0.05 * g * g
    step = m * lax.rsqrt(v + 1e-8) + 0.1 * w
    return (w - 0.02 * step).astype(BF), m, v


def owner(p, half, q):
    bits = ORDER[p]
    return half * bits[0] + q // 4 * bits[1] + q // 2 % 2 * bits[2] + q % 2 * bits[3]


def adamw_kernel(chunks, in_pieces, n_before, *refs):
    w, m, v = refs[0:3], refs[3:6], refs[6:9]
    n_g = 1 if in_pieces else 3
    g, outs = refs[9 : 9 + n_g], refs[9 + n_g + n_before : 18 + n_g + n_before]
    *bufs, load_sem, store_sem = refs[18 + n_g + n_before :]
    units, units_before = 2 * len(chunks), 2 * chunks[0]

    def window(ref, p, c, half):
        rows, columns = HALVES[p]
        layer, start = layer_and_start(c)
        if p < 2:
            return ref.at[layer, pl.ds(pl.multiple_of(half * rows, rows), rows), pl.ds(pl.multiple_of(start, 128), FC)]
        return ref.at[layer, pl.ds(pl.multiple_of(start + half * rows, 64), rows), :]

    def gradient(p, c, half, to, sem):
        if not in_pieces:
            return [pltpu.make_async_copy(window(g[p], p, c, half), to, sem)]
        copies = []
        for e in range(8):
            piece = g[0].at[owner(p, half, e), c - NG, p]
            if p < 2:
                copies.append(pltpu.make_async_copy(piece, to.at[pl.ds(64 * e, 64), :], sem))
            else:
                for b in range(5):
                    there = to.at[pl.ds(64 * b, 64), pl.ds(128 * e, 128)]
                    copies.append(pltpu.make_async_copy(piece.at[:, pl.ds(128 * b, 128)], there, sem))
        return copies

    def loads(n, act):
        (c, half), slot = split(n + units_before, 2), lax.rem(n, SLOTS)
        for p in range(3):
            for b, ref in enumerate((w[p], m[p], v[p])):
                copy = pltpu.make_async_copy(window(ref, p, c, half), bufs[4 * p + b].at[slot], load_sem.at[slot, p, b])
                copy.start() if act == "start" else copy.wait()
            to, sem = bufs[4 * p + 3].at[slot], load_sem.at[slot, p, 3]
            if act == "start":
                for copy in gradient(p, c, half, to, sem):
                    copy.start()
            else:
                pltpu.make_async_copy(window(w[p], p, c, half), to, sem).wait()

    def stores(n, act):
        (c, half), slot = split(n + units_before, 2), lax.rem(n, SLOTS)
        for p in range(3):
            for b in range(3):
                copy = pltpu.make_async_copy(bufs[4 * p + b].at[slot], window(outs[3 * b + p], p, c, half), store_sem.at[slot, p, b])
                copy.start() if act == "start" else copy.wait()

    loads(0, "start")
    loads(1, "start")

    def unit(n, carry):
        slot = lax.rem(n, SLOTS)

        @pl.when(n >= 2)
        def _():
            stores(n - 2, "wait")

        loads(n, "wait")

        @pl.when(n + 2 < units)
        def _():
            loads(n + 2, "start")

        for p in range(3):
            block = 64 if p < 2 else 32

            def rows_block(r, carry, buf=bufs[4 * p : 4 * p + 4], block=block):
                here = (slot, pl.ds(pl.multiple_of(r * block, block), block), slice(None))
                buf[0][here], buf[1][here], buf[2][here] = adamw(
                    buf[0][here].astype(F32), buf[1][here], buf[2][here], buf[3][here].astype(F32)
                )
                return carry

            lax.fori_loop(0, HALVES[p][0] // block, rows_block, 0)
        stores(n, "start")
        return carry

    lax.fori_loop(0, units, unit, 0)
    stores(units - 2, "wait")
    stores(units - 1, "wait")


def adamw_call(chunks, arrays, gradients, before=()):
    in_pieces, n_before = len(gradients) == 1, len(before)

    def kernel(*refs):
        adamw_kernel(chunks, in_pieces, n_before, *refs)

    elements, n_in = 3 * D * FC * len(chunks), 9 + len(gradients)
    return pl.pallas_call(
        kernel,
        out_shape=[jax.ShapeDtypeStruct(a.shape, a.dtype) for a in arrays],
        in_specs=any_spec(n_in + n_before),
        out_specs=any_spec(9),
        input_output_aliases={n_in + i: i for i in range(n_before)},
        scratch_shapes=[pltpu.VMEM((SLOTS, *shape), t) for shape in HALVES for t in (BF, F32, F32, BF)]
        + [pltpu.SemaphoreType.DMA((SLOTS, 3, 4)), pltpu.SemaphoreType.DMA((SLOTS, 3, 3))],
        compiler_params=pltpu.CompilerParams(vmem_limit_bytes=VMEM_LIMIT),
        cost_estimate=pl.CostEstimate(flops=15 * elements, bytes_accessed=22 * elements, transcendentals=elements),
        name="adamw_pieces" if in_pieces else "adamw_whole",
    )(*arrays, *gradients, *before)


def solution(mesh):
    def step(x, dy, *arrays):
        weights = arrays[:3]
        by0, hid0, h1, a1, a0 = forward(x[0], *weights)
        *gradients, pieces, _ = backward(a1, a0, dy[0], h1, by0, hid0, *weights)
        gathered = lax.all_gather(pieces, "dp")
        new = adamw_call(range(NG), arrays, gradients)
        return tuple(adamw_call(range(NG, NC), arrays, (gathered,), new))

    return jax.shard_map(
        step,
        mesh=mesh,
        in_specs=(P(("rep", "dp"), None, None),) * 2 + (P(None, None, None),) * 9,
        out_specs=(P("rep", None, None),) * 9,
        check_vma=False,
    )
```
